32 devices in a mesh: dom: 16 (over z, y, x), fault: 2 (over core).
Axes of the slice: x: 2, y: 2, z: 4, core: 2. Of those that a mesh axis runs over, the one named last changes fastest.
Arguments:
- modal_dofs: float32 [9, 56, 4096], P(None, None, ('dom', 'fault')), may hold values from -6 to 6
- star_matrices: float32 [3, 9, 9, 4096], P(None, None, None, ('dom', 'fault')), may hold values from -3.75 to 3.75
- stiffness: float32 [3, 56, 56], replicated, may hold values from -0.75 to 0.75
- face_proj: float32 [4, 56, 21], replicated, may hold values from -0.75 to 0.75
- face_flux: float32 [2, 4, 9, 9, 4096], P(None, None, None, None, ('dom', 'fault')), may hold values from -2 to 2
- neighbour_index: int32 [4, 4096], P(None, ('dom', 'fault')), may hold values from 0 to 767, as said below
- send_faces: int32 [4, 2048], P(None, ('dom', 'fault')), may hold values from 0 to 511, as said below
- fault_faces: int32 [12288], P(('dom', 'fault')), may hold values from 0 to 511, as said below
- fault_count: int32 [16], P('dom'), may hold values from 1 to 384, as said below
- fault_params: float32 [7, 21, 6144], P(None, None, 'dom'), may hold values from 0.03 to 6, as said below
- slip_guess: float32 [21, 6144], P(None, 'dom'), may hold values from 0.1 to 3
- fault_rotation: float32 [6, 9, 6144], P(None, None, 'dom'), may hold values from -2 to 2
- fault_flux: float32 [9, 6, 12288], P(None, None, ('dom', 'fault')), may hold values from -2.5 to 2.5
Outputs:
- new_dofs: float32 [9, 56, 4096], P(None, None, ('dom', 'fault'))
- slip_rate: float32 [21, 12288], P(None, ('dom', 'fault'))
- next_step: float32 [], replicated
The draws below stay inside these ranges and needn't reach their ends.
Inputs may be any that keep to these rules, and one draw needn't show every extreme that they name: `neighbour_index`: flat faces f * 128 + e of the partition. A value below 512 names a face of the same partition; a value v from 512 on names slot v - 512 of the received blocks in order of o, is carried by a face of an element below 64, and no slot is named twice in a partition. In every draw some partition names all 64 slots of some block. `send_faces`: flat faces of elements below 64 of the sending partition, all different within a partition. `fault_faces`: flat faces of the partition, all different within a partition. `fault_count`: the live slots of a chip are its first ones on both of its partitions; some chip has exactly 384. `fault_params`: Rows: a, state, normal_pre, shear_pre, length, zp, zs; all positive.
All inputs are finite; a program needn't handle non-finite values.
Results may differ from the reference program's by a relative error of at most 0.0003.
Values sent between devices are 32-bit elements; how exact they have to be, the bound alone decides.
A program may use at most 64 MiB of HBM per device.

```python
import math
import jax
import jax.numpy as jnp
from jax import lax

QUANT = 9
BASIS = 56
FACE_POINTS = 21
DERIVS = 6
NEWTON = 4
OFFS = 4
REACH = 8
ELEM_DEV = 128
PARTITIONS = 32
CHIPS = 16
EDGE = 64
BLOCK = 64
FMAX = 384
ELEMS = 4096
SLOTS = 12288
PAIR_SLOTS = 6144
N_DOM = 16


def halo_tables(key):
    boundary = EDGE
    block_size = BLOCK
    slots_all = OFFS * BLOCK

    def one_partition(part_index):
        base_key = jax.random.fold_in(jax.random.fold_in(key, 7331), part_index)
        subkeys = jax.random.split(base_key, 6)
        chosen = jax.random.permutation(subkeys[0], 4 * boundary)[:slots_all]
        send_rows = chosen // boundary * ELEM_DEV + chosen % boundary
        lowest = (2 * block_size + 4) // 5
        counts = jax.random.randint(subkeys[1], (OFFS,), lowest, block_size + 1)
        fullest = jax.random.randint(subkeys[2], (), 0, OFFS)
        counts = jnp.where(jnp.arange(OFFS) == fullest, block_size, counts)
        rank_keys = jax.random.split(subkeys[3], OFFS)
        slot_ranks = jnp.stack([jax.random.permutation(rank_keys[position], block_size) for position in range(OFFS)])
        live_flat = (slot_ranks < counts[:, None]).reshape(-1)
        takers = jax.random.permutation(subkeys[4], 4 * boundary)[:slots_all]
        taker_flat = takers // boundary * ELEM_DEV + takers % boundary
        local_faces = jax.random.randint(subkeys[5], (4 * ELEM_DEV,), 0, 4 * ELEM_DEV)
        remote = 4 * ELEM_DEV + jnp.arange(slots_all)
        face_table = local_faces.at[taker_flat].set(jnp.where(live_flat, remote, local_faces[taker_flat]))
        return (send_rows.reshape(OFFS, block_size).astype(jnp.int32), face_table.reshape(4, ELEM_DEV).astype(jnp.int32))
    return jax.vmap(one_partition)(jnp.arange(PARTITIONS))


def draw_star_matrices(key, part):
    subkeys = jax.random.split(jax.random.fold_in(key, 4421), 3)
    levels = jnp.exp(jax.random.uniform(subkeys[0], (PARTITIONS,), jnp.float32, math.log(0.6), math.log(4.5)))
    strongest = jax.random.randint(subkeys[1], (), 0, PARTITIONS)
    levels = jnp.where(jnp.arange(PARTITIONS) == strongest, 4.5, levels)
    grid_shape = (3, QUANT, QUANT, ELEMS)
    raw = jnp.clip(jax.random.normal(subkeys[2], grid_shape, jnp.float32), -2.5, 2.5)
    element_levels = jnp.repeat(levels, ELEM_DEV)
    return raw * element_levels[None, None, None, :] / 3.0


def draw_neighbour_index(key, part):
    send_rows, face_table = halo_tables(key)
    return jnp.transpose(face_table, (1, 0, 2)).reshape(4, ELEMS)


def draw_send_faces(key, part):
    send_rows, face_table = halo_tables(key)
    return jnp.transpose(send_rows, (1, 0, 2)).reshape(OFFS, BLOCK * PARTITIONS)


def draw_fault_faces(key, part):

    def one_device(part_index):
        subkey = jax.random.fold_in(jax.random.fold_in(key, 9157), part_index)
        return jax.random.permutation(subkey, 4 * ELEM_DEV)[:FMAX]
    return jax.vmap(one_device)(jnp.arange(PARTITIONS)).reshape(-1).astype(jnp.int32)


def draw_fault_count(key, part):
    subkeys = jax.random.split(jax.random.fold_in(key, 5113), 2)
    uniform_draws = jax.random.randint(subkeys[0], (CHIPS,), 0, 1000)
    counts = 1 + (FMAX - 1) * uniform_draws * uniform_draws // 998001
    fullest = jax.random.randint(subkeys[1], (), 0, CHIPS)
    return jnp.where(jnp.arange(CHIPS) == fullest, FMAX, counts).astype(jnp.int32)


def draw_fault_params(key, part):
    grid_shape = (FACE_POINTS, PAIR_SLOTS)
    subkeys = jax.random.split(jax.random.fold_in(key, 2719), 7)
    column = (jnp.arange(PAIR_SLOTS) // FMAX).astype(jnp.float32)
    trend_factor = 3.0 - 2.0 * column / max(CHIPS - 1, 1)

    def spread(subkey, lower_end, upper_end):
        return jnp.exp(jax.random.uniform(subkey, grid_shape, jnp.float32, math.log(lower_end), math.log(upper_end)))

    def evenly(subkey, lower_end, upper_end):
        return jax.random.uniform(subkey, grid_shape, jnp.float32, lower_end, upper_end)
    fric_a = spread(subkeys[0], 0.05, 0.2)
    state_value = evenly(subkeys[1], 0.4, 0.7)
    normal_pre = spread(subkeys[2], 0.2, 4.0)
    push_value = evenly(subkeys[3], -1.0, 2.0)
    length = spread(subkeys[4], 0.5, 2.0)
    shear_pre = normal_pre * (state_value + fric_a * push_value)
    imp_p = evenly(subkeys[5], 1.5, 3.0)
    imp_s = evenly(subkeys[6], 0.8, 1.6)
    return jnp.stack([fric_a, state_value, normal_pre, shear_pre, length * trend_factor[None, :], imp_p, imp_s])


def shard_levels(own_key, shape, cuts, least, high):
    level = 1.0
    for dim, blocks in cuts:
        draws = jax.random.uniform(jax.random.fold_in(jax.random.fold_in(own_key, 6), dim), (blocks,), jnp.float32, least / len(cuts), high / len(cuts))
        level = level * jnp.repeat(jnp.exp(draws), shape[dim] // blocks).reshape((-1,) + (1,) * (len(shape) - 1 - dim))
    return level


def noise(rng, extent, scale, most, cuts=(), held_as=jnp.bfloat16):
    factor_of = shard_levels(rng, extent, cuts, -0.22, 0.18) if cuts else 1.0
    values = jax.random.normal(rng, extent, jnp.float32) * scale * factor_of
    return jnp.minimum(jnp.maximum(values, -most), most).astype(held_as)


def setup_inputs(seed: int = 0) -> dict:
    streams_of = jax.random.split(jax.random.key(seed), 14)
    modal_dofs = noise(streams_of[0], (QUANT, BASIS, ELEMS), 1.0, 6.0, ((2, 32),), jnp.float32)
    star_matrices = draw_star_matrices(jax.random.fold_in(streams_of[13], 71), 0)
    stiffness = noise(streams_of[2], (3, BASIS, BASIS), BASIS ** -0.5, 0.75, (), jnp.float32)
    face_proj = noise(streams_of[3], (4, BASIS, FACE_POINTS), BASIS ** -0.5, 0.75, (), jnp.float32)
    face_flux = noise(streams_of[4], (2, 4, QUANT, QUANT, ELEMS), QUANT ** -0.5, 2.0, ((4, 32),), jnp.float32)
    neighbour_index = draw_neighbour_index(jax.random.fold_in(streams_of[13], 71), 0)
    send_faces = draw_send_faces(jax.random.fold_in(streams_of[13], 71), 0)
    fault_faces = draw_fault_faces(jax.random.fold_in(streams_of[13], 71), 0)
    fault_count = draw_fault_count(jax.random.fold_in(streams_of[13], 71), 0)
    fault_params = draw_fault_params(jax.random.fold_in(streams_of[13], 71), 0)
    slip_guess = jnp.clip(jnp.exp(math.log(3.0) - 3.4011974 * jax.random.uniform(streams_of[10], (FACE_POINTS, PAIR_SLOTS), jnp.float32) ** shard_levels(streams_of[10], (FACE_POINTS, PAIR_SLOTS), ((1, 16),), -0.2, 0.2)), 0.1, 3.0)
    fault_rotation = noise(streams_of[11], (6, QUANT, PAIR_SLOTS), QUANT ** -0.5, 2.0, ((2, 16),), jnp.float32)
    fault_flux = noise(streams_of[12], (QUANT, 6, SLOTS), 6 ** -0.5, 2.5, ((2, 32),), jnp.float32)
    return dict(modal_dofs=modal_dofs, star_matrices=star_matrices, stiffness=stiffness, face_proj=face_proj, face_flux=face_flux, neighbour_index=neighbour_index, send_faces=send_faces, fault_faces=fault_faces, fault_count=fault_count, fault_params=fault_params, slip_guess=slip_guess, fault_rotation=fault_rotation, fault_flux=fault_flux)


DT_STEP = 0.15
FAR_BOUND = 1e+30
HIGHEST_PRECISION = lax.Precision.HIGHEST

def inverse_sinh(values):
    magnitude = jnp.abs(values)
    return jnp.sign(values) * jnp.log(magnitude + jnp.sqrt(1.0 + magnitude * magnitude))

def apply_small(matrix, values):
    summed = matrix[:, 0][:, None, :] * values[0][None]
    for column in range(1, matrix.shape[1]):
        summed = summed + matrix[:, column][:, None, :] * values[column][None]
    return summed

def derivative(values, star_matrices, stiffness):
    summed = jnp.zeros_like(values)
    for direction in range(3):
        blended = apply_small(star_matrices[direction], values)
        summed = summed + jnp.einsum('bc,qce->qbe', stiffness[direction], blended, precision=HIGHEST_PRECISION)
    return -summed

def integrate(modal_dofs, star_matrices, stiffness):
    current = modal_dofs
    factor = DT_STEP
    result = factor * modal_dofs
    for degree in range(1, DERIVS):
        current = derivative(current, star_matrices, stiffness)
        factor = factor * DT_STEP / (degree + 1)
        result = result + factor * current
    return result

def face_traces(integrated, face_proj):
    return jnp.stack([jnp.einsum('bp,qbe->qpe', face_proj[face_id], integrated, precision=HIGHEST_PRECISION) for face_id in range(4)], axis=2)

def lift_face(face_proj, face_id, values):
    return jnp.einsum('bp,qpe->qbe', face_proj[face_id], values, precision=HIGHEST_PRECISION)

def volume_term(integrated, star_matrices, stiffness):
    summed = jnp.zeros_like(integrated)
    for direction in range(3):
        blended = apply_small(star_matrices[direction], integrated)
        summed = summed + jnp.einsum('cb,qce->qbe', stiffness[direction], blended, precision=HIGHEST_PRECISION)
    return summed

def surface_term(traces, trace_pool, neighbour_index, face_flux, face_proj):
    summed = None
    for face_id in range(4):
        outer_trace = jnp.take(trace_pool, neighbour_index[face_id], axis=2)
        values = apply_small(face_flux[0, face_id], traces[:, :, face_id]) + apply_small(face_flux[1, face_id], outer_trace)
        lifted = lift_face(face_proj, face_id, values)
        summed = lifted if summed is None else summed + lifted
    return summed

def friction(plus_side, minus_side, params, slip_guess):
    fric_a = params[0]
    state_value = params[1]
    normal_pre = params[2]
    shear_pre = params[3]
    imp_p = params[5]
    imp_s = params[6]
    normal_hat = 0.5 * (plus_side[0] + minus_side[0]) + 0.5 * imp_p * (minus_side[3] - plus_side[3])
    locked = shear_pre + 0.5 * (plus_side[1] + minus_side[1]) + 0.5 * imp_s * (minus_side[4] - plus_side[4])
    dip_hat = 0.5 * (plus_side[2] + minus_side[2]) + 0.5 * imp_s * (minus_side[5] - plus_side[5])
    effective = jnp.maximum(normal_pre - normal_hat, 0.0)
    growth = 0.5 * jnp.exp(state_value / fric_a)
    slip_speed = slip_guess
    for repeat in range(NEWTON):
        scaled = slip_speed * growth
        mismatch = locked - 0.5 * imp_s * slip_speed - effective * fric_a * inverse_sinh(scaled)
        slope_value = -0.5 * imp_s - effective * fric_a * growth / jnp.sqrt(1.0 + scaled * scaled)
        slip_speed = slip_speed - mismatch / slope_value
    shear_hat = locked - shear_pre - 0.5 * imp_s * slip_speed
    return (normal_hat, shear_hat, dip_hat, slip_speed)

def hat_state(own_side, normal_hat, shear_hat, dip_hat, params, orient):
    imp_p = params[5]
    imp_s = params[6]
    return jnp.stack([normal_hat, shear_hat, dip_hat, own_side[3] + orient * (normal_hat - own_side[0]) / imp_p, own_side[4] + orient * (shear_hat - own_side[1]) / imp_s, own_side[5] + orient * (dip_hat - own_side[2]) / imp_s])

def fault_lift(hat_values, fault_flux, fault_faces, live_slots, face_proj, elements):
    flux_values = jnp.where(live_slots[None, None], apply_small(fault_flux, hat_values), 0.0)
    face_of = fault_faces // elements
    element_of = fault_faces % elements
    lifted = jnp.zeros((flux_values.shape[0], face_proj.shape[1], flux_values.shape[2]), flux_values.dtype)
    for face_id in range(4):
        chosen = (face_of == face_id).astype(flux_values.dtype)
        lifted = lifted + chosen * jnp.einsum('bp,qps->qbs', face_proj[face_id], flux_values, precision=HIGHEST_PRECISION)
    empty = jnp.zeros((flux_values.shape[0], face_proj.shape[1], elements), flux_values.dtype)
    return empty.at[:, :, element_of].add(lifted)

def partitions_of(array, partitions):
    leading = array.shape[:-1]
    return jnp.moveaxis(array.reshape(leading + (partitions, array.shape[-1] // partitions)), -2, 0)

def rotate_pair(rotation, side_pair):
    return jnp.stack([apply_small(rotation, side_pair[0]), apply_small(rotation, side_pair[1])])

def both_hats(frame_pair, normal_hat, shear_hat, dip_hat, params):
    return jnp.stack([hat_state(frame_pair[0], normal_hat, shear_hat, dip_hat, params, 1.0), hat_state(frame_pair[1], normal_hat, shear_hat, dip_hat, params, -1.0)])

def reference(modal_dofs, star_matrices, stiffness, face_proj, face_flux, neighbour_index, send_faces, fault_faces, fault_count, fault_params, slip_guess, fault_rotation, fault_flux):
    partitions = modal_dofs.shape[2] // ELEM_DEV
    chip_count = N_DOM
    dofs_parts = partitions_of(modal_dofs, partitions)
    star_parts = partitions_of(star_matrices, partitions)
    flux_parts = partitions_of(face_flux, partitions)
    index_parts = partitions_of(neighbour_index, partitions)
    send_parts = partitions_of(send_faces, partitions)
    fault_face_parts = partitions_of(fault_faces.reshape(1, -1), partitions)[:, 0]
    fault_flux_parts = partitions_of(fault_flux, partitions)
    params_chips = partitions_of(fault_params, chip_count)
    guess_chips = partitions_of(slip_guess, chip_count)
    rotation_chips = partitions_of(fault_rotation, chip_count)

    def first_pass(pieces):
        dofs_one, star_one, send_one, fault_one = pieces
        integrated = integrate(dofs_one, star_one, stiffness)
        traces = face_traces(integrated, face_proj)
        flat_traces = traces.reshape(traces.shape[0], traces.shape[1], -1)
        return (jnp.take(flat_traces, send_one.reshape(-1), axis=2), jnp.take(flat_traces, fault_one, axis=2))
    outgoing, fault_trace = lax.map(first_pass, (dofs_parts, star_parts, send_parts, fault_face_parts))
    blocks = []
    for position, distance in enumerate((1, -1, REACH, -REACH)):
        block_piece = outgoing[:, :, :, position * BLOCK:(position + 1) * BLOCK]
        blocks.append(jnp.roll(block_piece, distance, axis=0))
    received = jnp.concatenate(blocks, axis=3)
    side_pairs = fault_trace.reshape((chip_count, 2) + fault_trace.shape[1:])
    frames = jax.vmap(rotate_pair)(rotation_chips, side_pairs)
    normal_hat, shear_hat, dip_hat, slip_speed = jax.vmap(friction)(frames[:, 0], frames[:, 1], params_chips, guess_chips)
    hat_sides = jax.vmap(both_hats)(frames, normal_hat, shear_hat, dip_hat, params_chips)
    hat_sides = hat_sides.reshape((partitions,) + hat_sides.shape[2:])
    live_chips = jnp.arange(FMAX, dtype=jnp.int32)[None, :] < fault_count[:, None]
    live_parts = jnp.repeat(live_chips, 2, axis=0)

    def second_pass(pieces):
        dofs_one, star_one, flux_one, index_one, received_one, hat_one, fault_one, fault_flux_one, live_one = pieces
        integrated = integrate(dofs_one, star_one, stiffness)
        traces = face_traces(integrated, face_proj)
        flat_traces = traces.reshape(traces.shape[0], traces.shape[1], -1)
        trace_pool = jnp.concatenate([flat_traces, received_one], axis=2)
        update = volume_term(integrated, star_one, stiffness) - surface_term(traces, trace_pool, index_one, flux_one, face_proj)
        update = update - fault_lift(hat_one, fault_flux_one, fault_one, live_one, face_proj, ELEM_DEV)
        return dofs_one + update
    new_parts = lax.map(second_pass, (dofs_parts, star_parts, flux_parts, index_parts, received, hat_sides, fault_face_parts, fault_flux_parts, live_parts))
    new_dofs = jnp.moveaxis(new_parts, 0, -2).reshape(modal_dofs.shape)
    slip_masked = jnp.where(live_chips[:, None, :], slip_speed, 0.0)
    slip_both = jnp.stack([slip_masked, slip_masked], axis=1)
    slip_rate = jnp.transpose(slip_both, (2, 0, 1, 3)).reshape(FACE_POINTS, -1)
    next_step = jnp.min(jnp.where(live_chips[:, None, :], params_chips[:, 4] / (jnp.abs(slip_speed) + 1.0), FAR_BOUND))
    return (new_dofs, slip_rate, next_step)
```

```python
import functools

import jax
import jax.numpy as jnp
from jax import lax
from jax.experimental import pallas as pl
from jax.experimental.pallas import tpu as pltpu
from jax.sharding import PartitionSpec as P

DERIVS = 6
NEWTON = 4
REACH = 8
DT_STEP = 0.15
FAR_BOUND = 1e30
LANES = 128
VMEM_BYTES = 67043328
MESH = pl.DeviceIdType.MESH
F32 = jnp.float32
BF16 = jnp.bfloat16


def up(size, unit):
    return -(-size // unit) * unit


def dot(left, right):
    return jnp.dot(left, right, preferred_element_type=F32)


def split(values):
    high = values.astype(BF16)
    low = (values - high.astype(F32)).astype(BF16)
    return high, low


def stacked(values):
    high, low = split(values)
    return jnp.concatenate([high, low], axis=0)


def pick(pair, table):
    half = pair.shape[0] // 2
    both = dot(pair, table)
    return both[:half] + both[half:]


def wide(matrix, width):
    high = matrix.astype(BF16).astype(F32)
    turned = high + pltpu.roll(matrix - high, width, 1)
    return jnp.concatenate([turned, high], axis=1)[:, : 3 * width].astype(BF16)


def product(left_pair, right):
    high, low = split(right)
    half = left_pair.shape[0] // 2
    both = dot(left_pair, high)
    return (both[:half] + both[half:]) + dot(left_pair[:half], low)


def kernel(
    chips,
    cores,
    dofs_hbm,
    star_hbm,
    stiff_hbm,
    proj_hbm,
    flux_hbm,
    neigh_hbm,
    send_hbm,
    faces_hbm,
    count_hbm,
    par_hbm,
    guess_hbm,
    rot_hbm,
    fflux_hbm,
    out_ref,
    slip_ref,
    step_ref,
    dofs_ref,
    star_ref,
    stiff_ref,
    proj_ref,
    flux_ref,
    neigh_ref,
    send_ref,
    faces_ref,
    par_ref,
    guess_ref,
    rot_ref,
    fflux_ref,
    count_ref,
    load_sem,
    x_buf,
    z_buf,
    integ,
    trace,
    pads,
    rows_buf,
    small,
    own_c,
    other_c,
    frame,
    halo_out,
    halo_in,
    lifted,
    fvals,
    bound_out,
    bound_in,
    send_sem,
    recv_sem,
    fault_send,
    fault_recv,
    bound_send,
    bound_recv,
):
    quants, basis, elems = dofs_ref.shape
    points, faces, _ = proj_ref.shape
    slots = faces_ref.shape[0]
    blocks, block = send_ref.shape
    rows = up(points, 8)
    face_rows = LANES // faces
    deep = up(basis, 16)
    flat = faces * elems
    dom = lax.axis_index("dom")
    core = lax.axis_index("fault")
    total = chips * cores
    me = dom * cores + core
    shifts = (1, -1, REACH, -REACH)

    def device_at(shift):
        at = lax.rem(me + shift + total, total)
        return (at // cores, lax.rem(at, cores))

    def chip_at(shift):
        return (lax.rem(dom + shift, chips), core)

    partner = (dom, core + 1 - 2 * lax.rem(core, 2))

    loads = []
    for source, target in (
        (stiff_hbm, stiff_ref),
        (proj_hbm, proj_ref),
        (dofs_hbm, dofs_ref),
        (star_hbm, star_ref),
        (faces_hbm, faces_ref),
        (rot_hbm, rot_ref),
        (par_hbm, par_ref),
        (send_hbm, send_ref),
        (guess_hbm, guess_ref),
        (fflux_hbm, fflux_ref),
        (neigh_hbm, neigh_ref),
        (flux_hbm, flux_ref),
        (count_hbm, count_ref),
    ):
        loads.append(pltpu.make_async_copy(source, target, load_sem.at[len(loads)]))
    for load in loads[:4]:
        load.start()

    barrier = pltpu.get_barrier_semaphore()
    for shift in shifts:
        pl.semaphore_signal(barrier, inc=1, device_id=device_at(-shift), device_id_type=MESH)
    pl.semaphore_signal(barrier, inc=1, device_id=partner, device_id_type=MESH)

    def each_hop(step):
        if chips <= 32:
            for hop in range(1, chips):
                step(hop)
        else:
            lax.fori_loop(1, chips, lambda hop, carry: (step(hop), carry)[1], 0)

    def greet(hop):
        pl.semaphore_signal(barrier, inc=1, device_id=chip_at(hop), device_id_type=MESH)

    each_hop(greet)

    pads[...] = jnp.zeros(pads.shape, F32)
    rows_buf[...] = jnp.zeros(rows_buf.shape, F32)
    small[...] = jnp.zeros(small.shape, jnp.int32)
    loads[0].wait()
    for d in range(3):
        pads[d, 0:basis, 0:basis] = stiff_ref[d]
    stiff_wide = wide(-jnp.concatenate([pads[d, 0:deep] for d in range(3)], axis=0), deep)

    gap = jnp.zeros((deep - basis, LANES), F32)
    pairs = [tuple(range(q, min(q + 2, quants))) for q in range(0, quants, 2)]
    triples = [tuple(range(q, min(q + 3, quants))) for q in range(0, quants, 3)]

    def tall(per_q, group):
        joined = jnp.concatenate(
            [jnp.concatenate([per_q(q), gap], axis=0) for q in group], axis=1
        )
        high, low = split(joined)
        return jnp.concatenate([high, high, low], axis=0)

    def multiply(matrix, per_q, keep):
        for group in pairs:
            result = dot(matrix, tall(per_q, group))
            for n, q in enumerate(group):
                keep(q, result[:, n * elems : (n + 1) * elems])

    def keep_z(q, result):
        for d in range(3):
            z_buf[d, q] = result[d * deep : d * deep + basis]

    def apply_star(group):
        sums = [None] * len(group)
        for d in range(3):
            for j in range(quants):
                column = z_buf[d, j]
                for n, q in enumerate(group):
                    term = star_ref[q, j, d : d + 1, :] * column
                    sums[n] = term if sums[n] is None else sums[n] + term
        return sums

    loads[1].wait()
    for p in range(points):
        rows_buf[p * faces : (p + 1) * faces, 0:basis] = proj_ref[p]
    for f in range(faces):
        pads[3, f * face_rows : f * face_rows + rows] = rows_buf[pl.ds(f, rows, faces), :]
    trace_wide = wide(pads[3], deep)
    loads[2].wait()
    loads[3].wait()
    for load in loads[4:]:
        load.start()
    factor = DT_STEP
    for degree in range(1, DERIVS):
        if degree == 1:
            multiply(stiff_wide, lambda q: dofs_ref[q], keep_z)
        else:
            multiply(stiff_wide, lambda q: x_buf[q], keep_z)
        past = factor
        factor = factor * DT_STEP / (degree + 1)
        for group in triples:
            for q, fresh in zip(group, apply_star(group)):
                if degree < DERIVS - 1:
                    x_buf[q] = fresh
                base = past * dofs_ref[q] if degree == 1 else integ[q]
                integ[q] = base + factor * fresh

    for k in (4, 5, 6):
        loads[k].wait()
    trace[quants * rows :, :] = jnp.zeros((trace.shape[0] - quants * rows, flat), F32)

    def keep_trace(q, result):
        for f in range(faces):
            first = f * face_rows
            trace[q * rows : (q + 1) * rows, f * elems : (f + 1) * elems] = result[
                first : first + rows
            ]

    multiply(trace_wide, lambda q: integ[q], keep_trace)
    trace_split = stacked(trace[...])

    def table(keys, wanted):
        return jnp.where(keys == wanted, 1.0, 0.0).astype(BF16)

    fault_keys = lax.broadcasted_iota(jnp.int32, (flat, slots), 0)
    fault_table = table(fault_keys, faces_ref[...].reshape(1, slots))
    own_trace = pick(trace_split, fault_table)
    orient = jnp.where(core == 0, 1.0, -1.0).astype(F32)
    for k in range(6):
        summed = None
        for j in range(quants):
            term = rot_ref[j, k : k + 1, :] * own_trace[j * rows : (j + 1) * rows]
            summed = term if summed is None else summed + term
        frame[k] = summed
    for k in range(3):
        impedance = par_ref[5 if k == 0 else 6]
        own_c[k, 0:points] = frame[k, 0:points] - orient * impedance * frame[k + 3, 0:points]

    pl.semaphore_wait(barrier, len(shifts) + chips)
    to_partner = pltpu.make_async_remote_copy(
        src_ref=own_c,
        dst_ref=other_c,
        send_sem=fault_send,
        recv_sem=fault_recv,
        device_id=partner,
        device_id_type=MESH,
    )
    to_partner.start()

    loads[7].wait()
    small[0:blocks, 0:block] = send_ref[...]
    half_rows = trace.shape[0] // 2
    doubled = small[...] + pltpu.roll(small[...], block, 1)
    lane = lax.broadcasted_iota(jnp.int32, (half_rows, LANES), 1)
    block_keys = lax.broadcasted_iota(jnp.int32, (flat, blocks * LANES), 0)
    wanted = jnp.concatenate([doubled[o : o + 1] for o in range(blocks)], axis=1)
    chosen = pick(trace_split, table(block_keys, wanted))
    copies = []
    for o, shift in enumerate(shifts):
        part = chosen[:, o * LANES : (o + 1) * LANES]
        halo_out[o] = jnp.where(lane < block, part[:half_rows], part[half_rows:])
        copies.append(
            pltpu.make_async_remote_copy(
                src_ref=halo_out.at[o],
                dst_ref=halo_in.at[o],
                send_sem=send_sem.at[o],
                recv_sem=recv_sem.at[o],
                device_id=device_at(shift),
                device_id_type=MESH,
            )
        )
        copies[-1].start()

    turned = [jnp.transpose(pads[d])[0:deep] for d in range(3)]
    turned_wide = wide(jnp.concatenate(turned, axis=0), deep)
    multiply(turned_wide, lambda q: integ[q], keep_z)
    for group in triples:
        for q, fresh in zip(group, apply_star(group)):
            out_ref[q] = dofs_ref[q] + fresh

    loads[8].wait()
    loads[12].wait()
    to_partner.wait_recv()
    fric_a, state_value, normal_pre, shear_pre = (par_ref[k] for k in range(4))
    imp_p, imp_s = par_ref[5], par_ref[6]
    normal_hat = 0.5 * (own_c[0, 0:points] + other_c[0, 0:points])
    locked = shear_pre + 0.5 * (own_c[1, 0:points] + other_c[1, 0:points])
    dip_hat = 0.5 * (own_c[2, 0:points] + other_c[2, 0:points])
    effective = jnp.maximum(normal_pre - normal_hat, 0.0)
    growth = 0.5 * jnp.exp(state_value / fric_a)
    strength = effective * fric_a
    slip_speed = guess_ref[...]
    for _ in range(NEWTON):
        scaled = slip_speed * growth
        magnitude = jnp.abs(scaled)
        root = jnp.sqrt(1.0 + scaled * scaled)
        logged = jnp.log(magnitude + root)
        logged = jnp.where(scaled < 0.0, -logged, logged)
        mismatch = locked - 0.5 * imp_s * slip_speed - strength * logged
        slope_value = -0.5 * imp_s - strength * growth / root
        slip_speed = slip_speed - mismatch / slope_value
    shear_hat = locked - shear_pre - 0.5 * imp_s * slip_speed
    live = lax.broadcasted_iota(jnp.int32, (points, slots), 1) < count_ref[0]
    slip_ref[...] = jnp.where(live, slip_speed, 0.0)
    bound = jnp.where(live, par_ref[4] / (jnp.abs(slip_speed) + 1.0), FAR_BOUND)
    bound = jnp.min(jnp.min(bound, axis=0, keepdims=True), axis=1, keepdims=True)
    bound_out[...] = jnp.broadcast_to(bound, (1, LANES))

    def send_bound(hop):
        pltpu.make_async_remote_copy(
            src_ref=bound_out,
            dst_ref=bound_in.at[hop - 1],
            send_sem=bound_send,
            recv_sem=bound_recv,
            device_id=chip_at(hop),
            device_id_type=MESH,
        ).start()

    each_hop(send_bound)

    loads[9].wait()
    hats = [normal_hat, shear_hat, dip_hat]
    for k in range(3):
        impedance = imp_p if k == 0 else imp_s
        hats.append(
            frame[k + 3, 0:points] + orient * (hats[k] - frame[k, 0:points]) / impedance
        )
    fvals[...] = jnp.zeros(fvals.shape, F32)
    for q in range(quants):
        summed = None
        for k in range(6):
            term = fflux_ref[q, k : k + 1, :] * hats[k]
            summed = term if summed is None else summed + term
        fvals[q * rows : q * rows + points, :] = jnp.where(live, summed, 0.0)
    spread_pair = stacked(fvals[...])
    spread = lax.dot_general(
        spread_pair, fault_table, (((1,), (1,)), ((), ())), preferred_element_type=F32
    )
    half = spread.shape[0] // 2
    lifted[...] = spread[:half] + spread[half:]

    loads[10].wait()
    loads[11].wait()
    neighbour = jnp.concatenate([neigh_ref[f : f + 1, :] for f in range(faces)], axis=1)
    face_keys = lax.broadcasted_iota(jnp.int32, (flat, flat), 0)
    local_part = pick(trace_split, table(face_keys, neighbour))
    place = lax.broadcasted_iota(jnp.int32, (blocks * LANES, flat), 0)
    spot = lax.rem(place, LANES)
    slot_key = flat + place // LANES * block
    top_table = table(jnp.where(spot < block, slot_key + spot, -1), neighbour)
    low_table = table(jnp.where(spot < block, -1, slot_key + spot - block), neighbour)

    for copy in copies:
        copy.wait_recv()
    arrived = stacked(jnp.concatenate([halo_in[o] for o in range(blocks)], axis=1))
    outer = local_part + jnp.concatenate(
        [pick(arrived, top_table), pick(arrived, low_table)], axis=0
    )
    lift_pair = stacked(jnp.transpose(pads[3])[:deep])
    pieces = []
    for f in range(faces):
        columns = slice(f * elems, (f + 1) * elems)
        values = []
        for q in range(quants):
            summed = lifted[q * rows : (q + 1) * rows, columns]
            for j in range(quants):
                inner = trace[j * rows : (j + 1) * rows, columns]
                near = outer[j * rows : (j + 1) * rows, columns]
                summed = summed + flux_ref[0, q, j, f : f + 1, :] * inner
                summed = summed + flux_ref[1, q, j, f : f + 1, :] * near
            values.append(summed)
        pieces.append(values)
    rest = jnp.zeros((face_rows - rows, LANES), F32)
    for group in pairs:
        columns = [
            jnp.concatenate(
                [part for f in range(faces) for part in (pieces[f][q], rest)], axis=0
            )
            for q in group
        ]
        result = product(lift_pair, jnp.concatenate(columns, axis=1))[:basis]
        for n, q in enumerate(group):
            out_ref[q] = out_ref[q] - result[:, n * elems : (n + 1) * elems]

    to_partner.wait_send()
    for copy in copies:
        copy.wait_send()
    best = bound_out[...]
    if chips > 1:
        pltpu.make_async_copy(bound_in, bound_in, bound_send).wait()
        pltpu.make_async_copy(bound_in, bound_in, bound_recv).wait()
        best = jnp.minimum(best, jnp.min(bound_in[...], axis=0))
    step_ref[...] = jnp.broadcast_to(best, step_ref.shape)


def store(dofs, slip, step, dofs_out, slip_out, step_out, least, sems):
    least[...] = step[0:1, 0:1]
    moves = ((dofs, dofs_out), (slip, slip_out), (least, step_out))
    copies = [pltpu.make_async_copy(a, b, sems.at[n]) for n, (a, b) in enumerate(moves)]
    for copy in copies:
        copy.start()
    for copy in copies:
        copy.wait()


def solution(mesh):
    chips, cores = mesh.shape["dom"], mesh.shape["fault"]
    hops = max(1, chips - 1)

    def on_device(
        modal_dofs,
        star_matrices,
        stiffness,
        face_proj,
        face_flux,
        neighbour_index,
        send_faces,
        fault_faces,
        fault_count,
        fault_params,
        slip_guess,
        fault_rotation,
        fault_flux,
    ):
        quants, basis, elems = modal_dofs.shape
        faces, _, points = face_proj.shape
        slots = fault_faces.shape[0]
        blocks = send_faces.shape[0]
        rows = up(points, 8)
        trace_rows = up(quants * rows, 32)
        star_matrices = jnp.transpose(star_matrices, (1, 2, 0, 3))
        face_proj = jnp.transpose(face_proj, (2, 0, 1))
        face_flux = jnp.transpose(face_flux, (0, 2, 3, 1, 4))
        fault_rotation = jnp.transpose(fault_rotation, (1, 0, 2))
        loaded = (
            modal_dofs,
            star_matrices,
            stiffness,
            face_proj,
            face_flux,
            neighbour_index,
            send_faces,
            fault_faces,
            fault_params,
            slip_guess,
            fault_rotation,
            fault_flux,
        )
        held = 4 * (quants * up(basis, 8) * elems + (rows + 8) * slots)
        vmem = pl.BlockSpec(memory_space=pltpu.VMEM)
        hbm = pl.BlockSpec(memory_space=pl.ANY)
        new_dofs, slip_rate, next_step = pl.pallas_call(
            functools.partial(kernel, chips, cores),
            out_shape=(
                pltpu.VMEM(modal_dofs.shape, F32),
                pltpu.VMEM(slip_guess.shape, F32),
                pltpu.VMEM((8, LANES), F32),
            ),
            in_specs=[hbm] * 13,
            out_specs=(vmem, vmem, vmem),
            scratch_shapes=[
                *(pltpu.VMEM(array.shape, array.dtype) for array in loaded),
                pltpu.SMEM(fault_count.shape, fault_count.dtype),
                pltpu.SemaphoreType.DMA((len(loaded) + 1,)),
                pltpu.VMEM((quants, basis, elems), F32),
                pltpu.VMEM((3, quants, basis, elems), F32),
                pltpu.VMEM((quants, basis, elems), F32),
                pltpu.VMEM((trace_rows, faces * elems), F32),
                pltpu.VMEM((4, LANES, LANES), F32),
                pltpu.VMEM((up(rows * faces, 8), LANES), F32),
                pltpu.VMEM((up(blocks, 8), LANES), jnp.int32),
                pltpu.VMEM((3, points, slots), F32),
                pltpu.VMEM((3, points, slots), F32),
                pltpu.VMEM((6, rows, slots), F32),
                pltpu.VMEM((blocks, trace_rows // 2, LANES), F32),
                pltpu.VMEM((blocks, trace_rows // 2, LANES), F32),
                pltpu.VMEM((trace_rows, faces * elems), F32),
                pltpu.VMEM((trace_rows, slots), F32),
                pltpu.VMEM((1, LANES), F32),
                pltpu.VMEM((hops, 1, LANES), F32),
                pltpu.SemaphoreType.DMA((blocks,)),
                pltpu.SemaphoreType.DMA((blocks,)),
                pltpu.SemaphoreType.DMA,
                pltpu.SemaphoreType.DMA,
                pltpu.SemaphoreType.DMA,
                pltpu.SemaphoreType.DMA,
            ],
            compiler_params=pltpu.CompilerParams(
                collective_id=0, has_side_effects=True, vmem_limit_bytes=VMEM_BYTES - held
            ),
        )(
            modal_dofs,
            star_matrices,
            stiffness,
            face_proj,
            face_flux,
            neighbour_index,
            send_faces,
            fault_faces,
            fault_count,
            fault_params,
            slip_guess,
            fault_rotation,
            fault_flux,
        )
        results = (new_dofs, slip_rate, next_step)
        new_dofs, slip_rate, next_step = pl.pallas_call(
            store,
            out_shape=(
                jax.ShapeDtypeStruct(new_dofs.shape, F32),
                jax.ShapeDtypeStruct(slip_rate.shape, F32),
                jax.ShapeDtypeStruct((1, 1), F32),
            ),
            in_specs=[vmem] * len(results),
            out_specs=(hbm,) * len(results),
            scratch_shapes=[pltpu.VMEM((1, 1), F32), pltpu.SemaphoreType.DMA((len(results),))],
            compiler_params=pltpu.CompilerParams(vmem_limit_bytes=4 * 1024 * 1024),
        )(*results)
        return new_dofs, slip_rate, next_step.reshape(())

    return jax.shard_map(
        on_device,
        mesh=mesh,
        in_specs=(
            P(None, None, ("dom", "fault")),
            P(None, None, None, ("dom", "fault")),
            P(),
            P(),
            P(None, None, None, None, ("dom", "fault")),
            P(None, ("dom", "fault")),
            P(None, ("dom", "fault")),
            P(("dom", "fault")),
            P("dom"),
            P(None, None, "dom"),
            P(None, "dom"),
            P(None, None, "dom"),
            P(None, None, ("dom", "fault")),
        ),
        out_specs=(P(None, None, ("dom", "fault")), P(None, ("dom", "fault")), P()),
        check_vma=False,
    )
```

```python
import functools

import jax
import jax.numpy as jnp
from jax import lax
from jax.experimental import pallas as pl
from jax.experimental.pallas import tpu as pltpu
from jax.sharding import PartitionSpec as P

DERIVS = 6
NEWTON = 4
REACH = 8
DT_STEP = 0.15
FAR_BOUND = 1e30
LANES = 128
EDGE = 64
VMEM_BYTES = 67043328
MESH = pl.DeviceIdType.MESH
F32 = jnp.float32
BF16 = jnp.bfloat16


def up(size, unit):
    return -(-size // unit) * unit


def dot(left, right):
    return jnp.dot(left, right, preferred_element_type=F32)


def split(values):
    high = values.astype(BF16)
    low = (values - high.astype(F32)).astype(BF16)
    return high, low


def stacked(values):
    high, low = split(values)
    return jnp.concatenate([high, low], axis=0)


def pick(pair, table):
    half = pair.shape[0] // 2
    both = dot(pair, table)
    return both[:half] + both[half:]


def pick_apart(pair, table):
    half = pair.shape[0] // 2
    return dot(pair[:half], table) + dot(pair[half:], table)


def wide(matrix, width):
    high = matrix.astype(BF16).astype(F32)
    turned = high + pltpu.roll(matrix - high, width, 1)
    return jnp.concatenate([turned, high], axis=1)[:, : 3 * width].astype(BF16)


def kernel(
    chips,
    cores,
    dofs_hbm,
    star_hbm,
    stiff_hbm,
    proj_hbm,
    flux_hbm,
    neigh_hbm,
    send_hbm,
    faces_hbm,
    count_hbm,
    par_hbm,
    guess_hbm,
    rot_hbm,
    fflux_hbm,
    out_ref,
    slip_ref,
    step_ref,
    dofs_ref,
    star_ref,
    stiff_ref,
    proj_ref,
    flux_ref,
    neigh_ref,
    send_ref,
    faces_ref,
    par_ref,
    guess_ref,
    rot_ref,
    fflux_ref,
    count_ref,
    load_sem,
    x_buf,
    z_buf,
    integ,
    trace,
    pads,
    rows_buf,
    small,
    own_c,
    other_c,
    frame,
    halo_out,
    halo_in,
    lifted,
    fvals,
    vals,
    pair_flux,
    bound_out,
    bound_in,
    send_sem,
    recv_sem,
    fault_send,
    fault_recv,
    bound_send,
    bound_recv,
):
    quants, basis, elems = dofs_ref.shape
    points, faces, _ = proj_ref.shape
    slots = faces_ref.shape[0]
    blocks, block = send_ref.shape
    rows = up(points, 8)
    face_rows = LANES // faces
    deep = up(basis, 16)
    flat = faces * elems
    dom = lax.axis_index("dom")
    core = lax.axis_index("fault")
    total = chips * cores
    me = dom * cores + core
    shifts = (1, -1, REACH, -REACH)

    def device_at(shift):
        at = lax.rem(me + shift + total, total)
        return (at // cores, lax.rem(at, cores))

    def chip_at(shift):
        return (lax.rem(dom + shift, chips), core)

    partner = (dom, core + 1 - 2 * lax.rem(core, 2))

    def load(source, target):
        copy = pltpu.make_async_copy(source, target, load_sem.at[len(loads)])
        loads.append(copy)
        return copy

    loads = []
    first = [
        load(source, target)
        for source, target in (
            (stiff_hbm, stiff_ref),
            (proj_hbm, proj_ref),
            (dofs_hbm, dofs_ref),
            (star_hbm, star_ref),
        )
    ]
    later = [
        load(source, target)
        for source, target in (
            (faces_hbm, faces_ref),
            (rot_hbm, rot_ref),
            *((par_hbm.at[k], par_ref.at[k]) for k in (5, 6)),
            (send_hbm, send_ref),
            *((par_hbm.at[k], par_ref.at[k]) for k in range(5)),
            (guess_hbm, guess_ref),
            (count_hbm, count_ref),
            (fflux_hbm, fflux_ref),
            (neigh_hbm, neigh_ref),
            (flux_hbm.at[0], flux_ref.at[0]),
            (flux_hbm.at[1], flux_ref.at[1]),
        )
    ]
    for copy in first:
        copy.start()
    waiting = list(later)

    def fence():
        if waiting:
            waiting.pop(0).wait()

    def arrived(number):
        while len(later) - len(waiting) < number:
            fence()

    barrier = pltpu.get_barrier_semaphore()
    for shift in shifts:
        pl.semaphore_signal(barrier, inc=1, device_id=device_at(-shift), device_id_type=MESH)
    pl.semaphore_signal(barrier, inc=1, device_id=partner, device_id_type=MESH)

    def each_hop(step):
        if chips <= 32:
            for hop in range(1, chips):
                step(hop)
        else:
            lax.fori_loop(1, chips, lambda hop, carry: (step(hop), carry)[1], 0)

    def greet(hop):
        pl.semaphore_signal(barrier, inc=1, device_id=chip_at(hop), device_id_type=MESH)

    each_hop(greet)

    pads[...] = jnp.zeros(pads.shape, F32)
    rows_buf[...] = jnp.zeros(rows_buf.shape, F32)
    small[...] = jnp.zeros(small.shape, jnp.int32)
    vals[...] = jnp.zeros(vals.shape, F32)
    first[0].wait()
    for copy in later:
        copy.start()
    for d in range(3):
        pads[d, 0:basis, 0:basis] = stiff_ref[d]
    stiff_wide = wide(-jnp.concatenate([pads[d, 0:deep] for d in range(3)], axis=0), deep)

    gap = jnp.zeros((deep - basis, LANES), F32)
    triples = [tuple(range(q, min(q + 3, quants))) for q in range(0, quants, 3)]

    def tall(per_q, group):
        joined = jnp.concatenate(
            [jnp.concatenate([per_q(q), gap], axis=0) for q in group], axis=1
        )
        high, low = split(joined)
        return jnp.concatenate([high, high, low], axis=0)

    def multiply(matrix, per_q, keep, group):
        result = dot(matrix, tall(per_q, group))
        for n, q in enumerate(group):
            keep(q, result[:, n * elems : (n + 1) * elems])

    def keep_z(at):
        def keep(q, result):
            for d in range(3):
                z_buf[at, d, q] = result[d * deep : d * deep + basis]

        return keep

    def keep_trace(q, result):
        for f in range(faces):
            first_row = f * face_rows
            trace[q * rows : (q + 1) * rows, f * elems : (f + 1) * elems] = result[
                first_row : first_row + rows
            ]

    def apply_star(at, group):
        sums = [None] * len(group)
        for j in range(quants):
            for d in range(3):
                column = z_buf[at, d, j]
                for n, q in enumerate(group):
                    term = star_ref[q, j, d : d + 1, :] * column
                    sums[n] = term if sums[n] is None else sums[n] + term
        return sums

    first[1].wait()
    for p in range(points):
        rows_buf[p * faces : (p + 1) * faces, 0:basis] = proj_ref[p]
    for f in range(faces):
        pads[3, f * face_rows : f * face_rows + rows] = rows_buf[pl.ds(f, rows, faces), :]
    trace_wide = wide(pads[3], deep)
    trace[quants * rows :, :] = jnp.zeros((trace.shape[0] - quants * rows, flat), F32)
    first[2].wait()
    for group in triples[:-1]:
        multiply(stiff_wide, lambda q: dofs_ref[q], keep_z(0), group)
    first[3].wait()
    factor = DT_STEP
    for degree in range(1, DERIVS):
        at, then = (degree - 1) % 2, degree % 2
        past = factor
        factor = factor * DT_STEP / (degree + 1)
        last = degree == DERIVS - 1
        for t, group in enumerate(triples):
            if t == 0:
                source = dofs_ref if degree == 1 else x_buf
                multiply(stiff_wide, lambda q: source[q], keep_z(at), triples[-1])
            elif last:
                multiply(trace_wide, lambda q: integ[q], keep_trace, triples[t - 1])
            else:
                multiply(stiff_wide, lambda q: x_buf[q], keep_z(then), triples[t - 1])
            for q, fresh in zip(group, apply_star(at, group)):
                if not last:
                    x_buf[q] = fresh
                base = past * dofs_ref[q] if degree == 1 else integ[q]
                integ[q] = base + factor * fresh
            if 1 < degree and t < len(triples) - 1:
                fence()
    multiply(trace_wide, lambda q: integ[q], keep_trace, triples[-1])
    trace_split = stacked(trace[...])

    def table(height, wanted, base=0):
        keys = lax.broadcasted_iota(jnp.int16, (height, wanted.shape[1]), 0)
        match = keys == (wanted - base).astype(jnp.int16)
        return jnp.where(match, jnp.array(1.0, BF16), jnp.array(0.0, BF16))

    arrived(4)
    fault_table = table(flat, faces_ref[...].reshape(1, slots))
    own_trace = pick(trace_split, fault_table)
    orient = jnp.where(core == 0, 1.0, -1.0).astype(F32)
    for k in range(6):
        summed = None
        for j in range(quants):
            term = rot_ref[j, k : k + 1, :] * own_trace[j * rows : (j + 1) * rows]
            summed = term if summed is None else summed + term
        frame[k] = summed
    for k in range(3):
        impedance = par_ref[5 if k == 0 else 6]
        own_c[k, 0:points] = frame[k, 0:points] - orient * impedance * frame[k + 3, 0:points]

    pl.semaphore_wait(barrier, len(shifts) + chips)
    def across(first_row, last_row, n):
        return pltpu.make_async_remote_copy(
            src_ref=own_c.at[first_row:last_row],
            dst_ref=other_c.at[first_row:last_row],
            send_sem=fault_send.at[n],
            recv_sem=fault_recv.at[n],
            device_id=partner,
            device_id_type=MESH,
        )

    to_partner = across(0, 2, 0)
    dip_over = across(2, 3, 1)
    to_partner.start()

    arrived(5)
    small[0:blocks, 0:block] = send_ref[...]
    half_rows = trace.shape[0] // 2
    lane = lax.broadcasted_iota(jnp.int32, (half_rows, LANES), 1)
    near_half = lane < block
    behind = pltpu.roll(small[...], block, 1)
    duos = range(0, blocks, 2)
    wanted = jnp.concatenate([small[o : o + 1] + behind[o + 1 : o + 2] for o in duos], axis=1)
    chosen = pick_apart(trace_split, table(flat, wanted))
    copies = []
    for o in duos:
        part = chosen[:, o // 2 * LANES : (o // 2 + 1) * LANES]
        upper, lower = part[:half_rows], part[half_rows:]
        halo_out[o] = jnp.where(near_half, upper, pltpu.roll(lower, block, 1))
        halo_out[o + 1] = jnp.where(near_half, pltpu.roll(upper, block, 1), lower)
    for o, shift in enumerate(shifts):
        copies.append(
            pltpu.make_async_remote_copy(
                src_ref=halo_out.at[o],
                dst_ref=halo_in.at[o],
                send_sem=send_sem.at[o],
                recv_sem=recv_sem.at[o],
                device_id=device_at(shift),
                device_id_type=MESH,
            )
        )
    for o in (0, 2):
        copies[o].start()

    turned = [jnp.transpose(pads[d])[0:deep] for d in range(3)]
    turned_wide = wide(jnp.concatenate(turned, axis=0), deep)
    for group in triples:
        multiply(turned_wide, lambda q: integ[q], keep_z(0), group)
    for group in triples:
        for q, fresh in zip(group, apply_star(0, group)):
            out_ref[q] = dofs_ref[q] + fresh
        fence()

    arrived(12)
    to_partner.wait_recv()
    fric_a, state_value, normal_pre, shear_pre = (par_ref[k] for k in range(4))
    imp_p, imp_s = par_ref[5], par_ref[6]
    normal_hat = 0.5 * (own_c[0, 0:points] + other_c[0, 0:points])
    locked = shear_pre + 0.5 * (own_c[1, 0:points] + other_c[1, 0:points])
    effective = jnp.maximum(normal_pre - normal_hat, 0.0)
    growth = 0.5 * jnp.exp(state_value / fric_a)
    strength = effective * fric_a
    slip_speed = guess_ref[...]
    for _ in range(NEWTON):
        scaled = slip_speed * growth
        magnitude = jnp.abs(scaled)
        root = jnp.sqrt(1.0 + scaled * scaled)
        logged = jnp.log(magnitude + root)
        logged = jnp.where(scaled < 0.0, -logged, logged)
        mismatch = locked - 0.5 * imp_s * slip_speed - strength * logged
        slope_value = -0.5 * imp_s - strength * growth / root
        slip_speed = slip_speed - mismatch / slope_value
    shear_hat = locked - shear_pre - 0.5 * imp_s * slip_speed
    live = lax.broadcasted_iota(jnp.int32, (points, slots), 1) < count_ref[0]
    slip_ref[...] = jnp.where(live, slip_speed, 0.0)
    bound = jnp.where(live, par_ref[4] / (jnp.abs(slip_speed) + 1.0), FAR_BOUND)
    bound = jnp.min(jnp.min(bound, axis=0, keepdims=True), axis=1, keepdims=True)
    bound_out[...] = jnp.broadcast_to(bound, (1, LANES))

    def send_bound(hop):
        pltpu.make_async_remote_copy(
            src_ref=bound_out,
            dst_ref=bound_in.at[hop - 1],
            send_sem=bound_send,
            recv_sem=bound_recv,
            device_id=chip_at(hop),
            device_id_type=MESH,
        ).start()

    each_hop(send_bound)
    for o in (1, 3):
        copies[o].start()
    dip_over.start()

    arrived(13)
    dip_over.wait_recv()
    dip_hat = 0.5 * (own_c[2, 0:points] + other_c[2, 0:points])
    hats = [normal_hat, shear_hat, dip_hat]
    for k in range(3):
        impedance = imp_p if k == 0 else imp_s
        hats.append(
            frame[k + 3, 0:points] + orient * (hats[k] - frame[k, 0:points]) / impedance
        )
    fvals[...] = jnp.zeros(fvals.shape, F32)
    for q in range(quants):
        summed = None
        for k in range(6):
            term = fflux_ref[q, k : k + 1, :] * hats[k]
            summed = term if summed is None else summed + term
        fvals[q * rows : q * rows + points, :] = jnp.where(live, summed, 0.0)
    spread_pair = stacked(fvals[...])
    spread = lax.dot_general(
        spread_pair, fault_table, (((1,), (1,)), ((), ())), preferred_element_type=F32
    )
    half = spread.shape[0] // 2
    lifted[...] = spread[:half] + spread[half:]

    arrived(len(later))
    neighbour = jnp.concatenate([neigh_ref[f : f + 1, :] for f in range(faces)], axis=1)
    local_part = pick(trace_split, table(flat, neighbour))
    lane_tile = lax.broadcasted_iota(jnp.int32, (faces, LANES), 1)
    wide_lane = lax.broadcasted_iota(jnp.int32, (basis, LANES), 1)
    duo_faces = range(0, faces, 2)

    def face_pairs(tile):
        shifted = pltpu.roll(jnp.concatenate([tile[1:], tile[:1]], axis=0), EDGE, 1)
        return jnp.where(lane_tile < EDGE, tile, shifted)

    paired = face_pairs(neigh_ref[...])
    far_keys = jnp.concatenate([paired[f : f + 1] for f in duo_faces], axis=1)
    far_table = table(blocks * block, far_keys, flat)
    for q in range(quants):
        for j in range(quants):
            pair_flux[q, j] = face_pairs(flux_ref[1, q, j])
    lift_pair = stacked(jnp.transpose(pads[3])[:deep])
    lift_wide = jnp.concatenate([lift_pair[:deep], lift_pair[deep:], lift_pair[:deep]], axis=1)
    for f in range(faces):
        columns = slice(f * elems, (f + 1) * elems)
        for q in range(quants):
            summed = lifted[q * rows : (q + 1) * rows, columns]
            for j in range(quants):
                inner = trace[j * rows : (j + 1) * rows, columns]
                near = local_part[j * rows : (j + 1) * rows, columns]
                summed = summed + flux_ref[0, q, j, f : f + 1, :] * inner
                summed = summed + flux_ref[1, q, j, f : f + 1, :] * near
            vals[q, f * face_rows : f * face_rows + rows] = summed

    def three(joined):
        high, low = split(joined)
        return jnp.concatenate([high, high, low], axis=0)

    for group in triples:
        result = dot(lift_wide, three(jnp.concatenate([vals[q] for q in group], axis=1)))
        for n, q in enumerate(group):
            out_ref[q] = out_ref[q] - result[:basis, n * elems : (n + 1) * elems]

    sorted_rows = jnp.concatenate(
        [pads[3, f * face_rows : (f + 1) * face_rows] for f in (*duo_faces, *range(1, faces, 2))],
        axis=0,
    )
    tall_lift = jnp.transpose(sorted_rows)[:deep]
    lift_lane = lax.broadcasted_iota(jnp.int32, (deep, LANES), 1)
    both_lifts = jnp.concatenate(
        [
            jnp.where(lift_lane < deep, tall_lift, 0.0),
            jnp.where(lift_lane < deep, pltpu.roll(tall_lift, LANES - deep, 1), 0.0),
        ],
        axis=0,
    )
    far_wide = wide(both_lifts, deep)

    for copy in copies:
        copy.wait_recv()
    columns = []
    for o in duos:
        upper, lower = halo_in[o], halo_in[o + 1]
        columns.append(
            jnp.concatenate(
                [
                    jnp.where(near_half, upper, pltpu.roll(lower, block, 1)),
                    jnp.where(near_half, pltpu.roll(upper, block, 1), lower),
                ],
                axis=0,
            )
        )
    far = pick(stacked(jnp.concatenate(columns, axis=1)), far_table)
    rest = jnp.zeros((face_rows - rows, LANES), F32)
    for group in triples:
        parts = []
        for q in group:
            pieces = []
            for c in range(len(duo_faces)):
                summed = None
                for j in range(quants):
                    term = pair_flux[q, j, 2 * c : 2 * c + 1, :] * far[
                        j * rows : (j + 1) * rows, c * LANES : (c + 1) * LANES
                    ]
                    summed = term if summed is None else summed + term
                pieces += [summed, rest]
            parts.append(jnp.concatenate(pieces, axis=0))
        result = dot(far_wide, three(jnp.concatenate(parts, axis=1)))
        for n, q in enumerate(group):
            even = result[:basis, n * elems : (n + 1) * elems]
            odd = result[deep : deep + basis, n * elems : (n + 1) * elems]
            both = even + pltpu.roll(odd, LANES - EDGE, 1)
            out_ref[q] = out_ref[q] - jnp.where(wide_lane < EDGE, both, 0.0)

    to_partner.wait_send()
    dip_over.wait_send()
    for copy in copies:
        copy.wait_send()
    best = bound_out[...]
    if chips > 1:
        pltpu.make_async_copy(bound_in, bound_in, bound_send).wait()
        pltpu.make_async_copy(bound_in, bound_in, bound_recv).wait()
        best = jnp.minimum(best, jnp.min(bound_in[...], axis=0))
    step_ref[...] = jnp.broadcast_to(best, step_ref.shape)


def store(dofs, slip, step, dofs_out, slip_out, step_out, least, sems):
    least[...] = step[0:1, 0:1]
    moves = ((dofs, dofs_out), (slip, slip_out), (least, step_out))
    copies = [pltpu.make_async_copy(a, b, sems.at[n]) for n, (a, b) in enumerate(moves)]
    for copy in copies:
        copy.start()
    for copy in copies:
        copy.wait()


def solution(mesh):
    chips, cores = mesh.shape["dom"], mesh.shape["fault"]
    hops = max(1, chips - 1)

    def on_device(
        modal_dofs,
        star_matrices,
        stiffness,
        face_proj,
        face_flux,
        neighbour_index,
        send_faces,
        fault_faces,
        fault_count,
        fault_params,
        slip_guess,
        fault_rotation,
        fault_flux,
    ):
        quants, basis, elems = modal_dofs.shape
        faces, _, points = face_proj.shape
        slots = fault_faces.shape[0]
        blocks = send_faces.shape[0]
        rows = up(points, 8)
        trace_rows = up(quants * rows, 32)
        star_matrices = jnp.transpose(star_matrices, (1, 2, 0, 3))
        face_proj = jnp.transpose(face_proj, (2, 0, 1))
        face_flux = jnp.transpose(face_flux, (0, 2, 3, 1, 4))
        fault_rotation = jnp.transpose(fault_rotation, (1, 0, 2))
        loaded = (
            modal_dofs,
            star_matrices,
            stiffness,
            face_proj,
            face_flux,
            neighbour_index,
            send_faces,
            fault_faces,
            fault_params,
            slip_guess,
            fault_rotation,
            fault_flux,
        )
        held = 4 * (quants * up(basis, 8) * elems + (rows + 8) * slots)
        vmem = pl.BlockSpec(memory_space=pltpu.VMEM)
        hbm = pl.BlockSpec(memory_space=pl.ANY)
        new_dofs, slip_rate, next_step = pl.pallas_call(
            functools.partial(kernel, chips, cores),
            out_shape=(
                pltpu.VMEM(modal_dofs.shape, F32),
                pltpu.VMEM(slip_guess.shape, F32),
                pltpu.VMEM((8, LANES), F32),
            ),
            in_specs=[hbm] * 13,
            out_specs=(vmem, vmem, vmem),
            scratch_shapes=[
                *(pltpu.VMEM(array.shape, array.dtype) for array in loaded),
                pltpu.SMEM(fault_count.shape, fault_count.dtype),
                pltpu.SemaphoreType.DMA((len(loaded) + fault_params.shape[0] + 1,)),
                pltpu.VMEM((quants, basis, elems), F32),
                pltpu.VMEM((2, 3, quants, basis, elems), F32),
                pltpu.VMEM((quants, basis, elems), F32),
                pltpu.VMEM((trace_rows, faces * elems), F32),
                pltpu.VMEM((4, LANES, LANES), F32),
                pltpu.VMEM((up(rows * faces, 8), LANES), F32),
                pltpu.VMEM((up(blocks, 8), LANES), jnp.int32),
                pltpu.VMEM((3, points, slots), F32),
                pltpu.VMEM((3, points, slots), F32),
                pltpu.VMEM((6, rows, slots), F32),
                pltpu.VMEM((blocks, trace_rows // 2, LANES), F32),
                pltpu.VMEM((blocks, trace_rows // 2, LANES), F32),
                pltpu.VMEM((trace_rows, faces * elems), F32),
                pltpu.VMEM((trace_rows, slots), F32),
                pltpu.VMEM((quants, LANES, elems), F32),
                pltpu.VMEM((quants, quants, faces, elems), F32),
                pltpu.VMEM((1, LANES), F32),
                pltpu.VMEM((hops, 1, LANES), F32),
                pltpu.SemaphoreType.DMA((blocks,)),
                pltpu.SemaphoreType.DMA((blocks,)),
                pltpu.SemaphoreType.DMA((2,)),
                pltpu.SemaphoreType.DMA((2,)),
                pltpu.SemaphoreType.DMA,
                pltpu.SemaphoreType.DMA,
            ],
            compiler_params=pltpu.CompilerParams(
                collective_id=0, has_side_effects=True, vmem_limit_bytes=VMEM_BYTES - held
            ),
        )(
            modal_dofs,
            star_matrices,
            stiffness,
            face_proj,
            face_flux,
            neighbour_index,
            send_faces,
            fault_faces,
            fault_count,
            fault_params,
            slip_guess,
            fault_rotation,
            fault_flux,
        )
        results = (new_dofs, slip_rate, next_step)
        new_dofs, slip_rate, next_step = pl.pallas_call(
            store,
            out_shape=(
                jax.ShapeDtypeStruct(new_dofs.shape, F32),
                jax.ShapeDtypeStruct(slip_rate.shape, F32),
                jax.ShapeDtypeStruct((1, 1), F32),
            ),
            in_specs=[vmem] * len(results),
            out_specs=(hbm,) * len(results),
            scratch_shapes=[pltpu.VMEM((1, 1), F32), pltpu.SemaphoreType.DMA((len(results),))],
            compiler_params=pltpu.CompilerParams(vmem_limit_bytes=4 * 1024 * 1024),
        )(*results)
        return new_dofs, slip_rate, next_step.reshape(())

    return jax.shard_map(
        on_device,
        mesh=mesh,
        in_specs=(
            P(None, None, ("dom", "fault")),
            P(None, None, None, ("dom", "fault")),
            P(),
            P(),
            P(None, None, None, None, ("dom", "fault")),
            P(None, ("dom", "fault")),
            P(None, ("dom", "fault")),
            P(("dom", "fault")),
            P("dom"),
            P(None, None, "dom"),
            P(None, "dom"),
            P(None, None, "dom"),
            P(None, None, ("dom", "fault")),
        ),
        out_specs=(P(None, None, ("dom", "fault")), P(None, ("dom", "fault")), P()),
        check_vma=False,
    )
```

```python
import functools

import jax
import jax.numpy as jnp
from jax import lax
from jax.experimental import pallas as pl
from jax.experimental.pallas import tpu as pltpu
from jax.sharding import PartitionSpec as P

DERIVS = 6
NEWTON = 4
REACH = 8
DT_STEP = 0.15
FAR_BOUND = 1e30
LANES = 128
EDGE = 64
VMEM_BYTES = 67043328
MESH = pl.DeviceIdType.MESH
F32 = jnp.float32
BF16 = jnp.bfloat16


def up(size, unit):
    return -(-size // unit) * unit


def dot(left, right):
    return jnp.dot(left, right, preferred_element_type=F32)


def split(values):
    high = values.astype(BF16)
    low = (values - high.astype(F32)).astype(BF16)
    return high, low


def stacked(values):
    high, low = split(values)
    return jnp.concatenate([high, low], axis=0)


def pick(pair, table):
    half = pair.shape[0] // 2
    both = dot(pair, table)
    return both[:half] + both[half:]


def wide(matrix, width):
    high = matrix.astype(BF16).astype(F32)
    turned = high + pltpu.roll(matrix - high, width, 1)
    return jnp.concatenate([turned, high], axis=1)[:, : 3 * width].astype(BF16)


def kernel(
    chips,
    cores,
    dofs_hbm,
    star_hbm,
    stiff_hbm,
    proj_hbm,
    flux_hbm,
    neigh_hbm,
    send_hbm,
    faces_hbm,
    count_hbm,
    par_hbm,
    guess_hbm,
    rot_hbm,
    fflux_hbm,
    out_ref,
    slip_ref,
    step_ref,
    dofs_ref,
    star_ref,
    stiff_ref,
    proj_ref,
    flux_ref,
    neigh_ref,
    send_ref,
    faces_ref,
    par_ref,
    guess_ref,
    rot_ref,
    fflux_ref,
    count_ref,
    load_sem,
    x_buf,
    z_buf,
    integ,
    trace,
    pads,
    rows_buf,
    small,
    own_c,
    other_c,
    own_dip,
    other_dip,
    own_trace,
    chosen,
    local_part,
    trace_parts,
    fault_table,
    send_table,
    frame,
    halo_out,
    halo_in,
    lifted,
    fvals,
    vals,
    pair_flux,
    bound_out,
    bound_in,
    send_sem,
    recv_sem,
    fault_send,
    fault_recv,
    bound_send,
    bound_recv,
):
    quants, basis, elems = dofs_ref.shape
    points, faces, _ = proj_ref.shape
    slots = faces_ref.shape[0]
    blocks, block = send_ref.shape
    rows = up(points, 8)
    face_rows = LANES // faces
    deep = up(basis, 16)
    flat = faces * elems
    dom = lax.axis_index("dom")
    core = lax.axis_index("fault")
    total = chips * cores
    me = dom * cores + core
    shifts = (1, -1, REACH, -REACH)

    def device_at(shift):
        at = lax.rem(me + shift + total, total)
        return (at // cores, lax.rem(at, cores))

    def chip_at(shift):
        return (lax.rem(dom + shift, chips), core)

    partner = (dom, core + 1 - 2 * lax.rem(core, 2))

    def load(source, target):
        copy = pltpu.make_async_copy(source, target, load_sem.at[len(loads)])
        loads.append(copy)
        return copy

    loads = []
    first = [
        load(source, target)
        for source, target in (
            (stiff_hbm, stiff_ref),
            (proj_hbm, proj_ref),
            (dofs_hbm, dofs_ref),
            (star_hbm, star_ref),
        )
    ]
    later = [
        load(source, target)
        for source, target in (
            (faces_hbm, faces_ref),
            (send_hbm, send_ref),
            (rot_hbm, rot_ref),
            *((par_hbm.at[k], par_ref.at[k]) for k in (5, 6)),
            *((par_hbm.at[k], par_ref.at[k]) for k in range(5)),
            (guess_hbm, guess_ref),
            (count_hbm, count_ref),
            (fflux_hbm, fflux_ref),
            (neigh_hbm, neigh_ref),
            (flux_hbm.at[0], flux_ref.at[0]),
            (flux_hbm.at[1], flux_ref.at[1]),
        )
    ]
    for copy in first + later:
        copy.start()
    waiting = list(later)

    def fence():
        if waiting:
            waiting.pop(0).wait()

    def arrived(number):
        while len(later) - len(waiting) < number:
            fence()

    barrier = pltpu.get_barrier_semaphore()
    for shift in shifts:
        pl.semaphore_signal(barrier, inc=1, device_id=device_at(-shift), device_id_type=MESH)
    pl.semaphore_signal(barrier, inc=1, device_id=partner, device_id_type=MESH)

    def each_hop(step):
        if chips <= 32:
            for hop in range(1, chips):
                step(hop)
        else:
            lax.fori_loop(1, chips, lambda hop, carry: (step(hop), carry)[1], 0)

    def greet(hop):
        pl.semaphore_signal(barrier, inc=1, device_id=chip_at(hop), device_id_type=MESH)

    each_hop(greet)

    pads[...] = jnp.zeros(pads.shape, F32)
    rows_buf[...] = jnp.zeros(rows_buf.shape, F32)
    small[...] = jnp.zeros(small.shape, jnp.int32)
    vals[...] = jnp.zeros(vals.shape, F32)
    chosen[quants * rows :, :] = jnp.zeros((chosen.shape[0] - quants * rows, chosen.shape[1]), F32)
    first[0].wait()
    for d in range(3):
        pads[d, 0:basis, 0:basis] = stiff_ref[d]
    stiff_wide = wide(-jnp.concatenate([pads[d, 0:deep] for d in range(3)], axis=0), deep)

    gap = jnp.zeros((deep - basis, LANES), F32)
    triples = [tuple(range(q, min(q + 3, quants))) for q in range(0, quants, 3)]

    def tall(per_q, group):
        joined = jnp.concatenate(
            [jnp.concatenate([per_q(q), gap], axis=0) for q in group], axis=1
        )
        high, low = split(joined)
        return jnp.concatenate([high, high, low], axis=0)

    def multiply(matrix, per_q, keep, group):
        result = dot(matrix, tall(per_q, group))
        for n, q in enumerate(group):
            keep(q, result[:, n * elems : (n + 1) * elems])

    def keep_z(at):
        def keep(q, result):
            for d in range(3):
                z_buf[at, d, q] = result[d * deep : d * deep + basis]

        return keep

    def keep_trace(q, result):
        for f in range(faces):
            first_row = f * face_rows
            trace[q * rows : (q + 1) * rows, f * elems : (f + 1) * elems] = result[
                first_row : first_row + rows
            ]

    def apply_star(at, group):
        sums = [None] * len(group)
        for j in range(quants):
            for d in range(3):
                column = z_buf[at, d, j]
                for n, q in enumerate(group):
                    term = star_ref[q, j, d : d + 1, :] * column
                    sums[n] = term if sums[n] is None else sums[n] + term
        return sums

    first[1].wait()
    for p in range(points):
        rows_buf[p * faces : (p + 1) * faces, 0:basis] = proj_ref[p]
    for f in range(faces):
        pads[3, f * face_rows : f * face_rows + rows] = rows_buf[pl.ds(f, rows, faces), :]
    trace_wide = wide(pads[3], deep)
    trace[quants * rows :, :] = jnp.zeros((trace.shape[0] - quants * rows, flat), F32)
    first[2].wait()
    for group in triples[:-1]:
        multiply(stiff_wide, lambda q: dofs_ref[q], keep_z(0), group)
    first[3].wait()

    def table(height, wanted, base=0):
        keys = lax.broadcasted_iota(jnp.int16, (height, wanted.shape[1]), 0)
        match = keys == (wanted - base).astype(jnp.int16)
        return jnp.where(match, jnp.array(1.0, BF16), jnp.array(0.0, BF16))

    duos = range(0, blocks, 2)

    def build_tables():
        arrived(2)
        fault_table[...] = table(flat, faces_ref[...].reshape(1, slots))
        small[0:blocks, 0:block] = send_ref[...]
        behind = pltpu.roll(small[...], block, 1)
        wanted = jnp.concatenate(
            [small[o : o + 1] + behind[o + 1 : o + 2] for o in duos], axis=1
        )
        send_table[...] = table(flat, wanted)

    tier = trace_parts.shape[0] // (2 * len(triples))

    def split_trace(g):
        height = len(triples[g]) * rows
        base = triples[g][0] * rows
        spare = jnp.zeros((tier - height, flat), F32)
        both = stacked(jnp.concatenate([trace[base : base + height, :], spare], axis=0))
        trace_parts[2 * g * tier : 2 * (g + 1) * tier] = both

    def place(both, g, target):
        height = len(triples[g]) * rows
        base = triples[g][0] * rows
        target[base : base + height, :] = both[:height] + both[tier : tier + height]

    def pick_group(g, chosen_table, target):
        place(dot(trace_parts[2 * g * tier : 2 * (g + 1) * tier], chosen_table), g, target)

    def pick_all(chosen_table, target):
        both = dot(trace_parts[...], chosen_table)
        for g in range(len(triples)):
            place(both[2 * g * tier : 2 * (g + 1) * tier], g, target)

    factor = DT_STEP
    for degree in range(1, DERIVS):
        at, then = (degree - 1) % 2, degree % 2
        past = factor
        factor = factor * DT_STEP / (degree + 1)
        last = degree == DERIVS - 1
        if last:
            build_tables()
        for t, group in enumerate(triples):
            if t == 0:
                source = dofs_ref if degree == 1 else x_buf
                multiply(stiff_wide, lambda q: source[q], keep_z(at), triples[-1])
            elif last:
                multiply(trace_wide, lambda q: integ[q], keep_trace, triples[t - 1])
                if t > 1:
                    split_trace(t - 2)
            else:
                multiply(stiff_wide, lambda q: x_buf[q], keep_z(then), triples[t - 1])
            for q, fresh in zip(group, apply_star(at, group)):
                if not last:
                    x_buf[q] = fresh
                base = past * dofs_ref[q] if degree == 1 else integ[q]
                integ[q] = base + factor * fresh
            if t < len(triples) - 1:
                fence()
    multiply(trace_wide, lambda q: integ[q], keep_trace, triples[-1])
    split_trace(len(triples) - 2)
    split_trace(len(triples) - 1)
    pick_all(fault_table[...], own_trace)
    orient = jnp.where(core == 0, 1.0, -1.0).astype(F32)
    chunks = [slice(c * LANES, (c + 1) * LANES) for c in range(slots // LANES)]
    arrived(5)

    def turn(k, lanes):
        summed = None
        for j in range(quants):
            term = rot_ref[j, k : k + 1, lanes] * own_trace[j * rows : (j + 1) * rows, lanes]
            summed = term if summed is None else summed + term
        frame[k, :, lanes] = summed
        return summed[:points]

    def face_both(k, lanes):
        impedance = par_ref[5 if k == 0 else 6, :, lanes]
        stress, speed = turn(k, lanes), turn(k + 3, lanes)
        return stress - orient * impedance * speed

    def across(c):
        return pltpu.make_async_remote_copy(
            src_ref=own_c.at[c],
            dst_ref=other_c.at[c],
            send_sem=fault_send.at[c],
            recv_sem=fault_recv.at[c],
            device_id=partner,
            device_id_type=MESH,
        )

    crossing = [across(c) for c in range(len(chunks))]
    dip_over = pltpu.make_async_remote_copy(
        src_ref=own_dip,
        dst_ref=other_dip,
        send_sem=fault_send.at[len(chunks)],
        recv_sem=fault_recv.at[len(chunks)],
        device_id=partner,
        device_id_type=MESH,
    )
    for c, lanes in enumerate(chunks):
        for k in range(2):
            own_c[c, k] = face_both(k, lanes)
        if c == 0:
            pl.semaphore_wait(barrier, len(shifts) + chips)
        crossing[c].start()

    pick_all(send_table[...], chosen)
    half_rows = trace.shape[0] // 2
    lane = lax.broadcasted_iota(jnp.int32, (half_rows, LANES), 1)
    near_half = lane < block
    copies = []
    for o in duos:
        lanes = slice(o // 2 * LANES, (o // 2 + 1) * LANES)
        upper, lower = chosen[:half_rows, lanes], chosen[half_rows:, lanes]
        halo_out[o] = jnp.where(near_half, upper, pltpu.roll(lower, block, 1))
        halo_out[o + 1] = jnp.where(near_half, pltpu.roll(upper, block, 1), lower)
    for o, shift in enumerate(shifts):
        copies.append(
            pltpu.make_async_remote_copy(
                src_ref=halo_out.at[o],
                dst_ref=halo_in.at[o],
                send_sem=send_sem.at[o],
                recv_sem=recv_sem.at[o],
                device_id=device_at(shift),
                device_id_type=MESH,
            )
        )
    urgent = [lax.rem(me + shift + total, total) < cores for shift in shifts]

    def start_if(wanted):
        for copy, first_of_all in zip(copies, urgent):
            pl.when(first_of_all == wanted)(copy.start)

    start_if(True)
    for lanes in chunks:
        own_dip[:, lanes] = face_both(2, lanes)

    arrived(12)
    least = None
    faced = []
    for c, lanes in enumerate(chunks):
        crossing[c].wait_recv()
        fric_a, state_value, normal_pre, shear_pre = (par_ref[k, :, lanes] for k in range(4))
        imp_s = par_ref[6, :, lanes]
        normal_hat = 0.5 * (own_c[c, 0] + other_c[c, 0])
        locked = shear_pre + 0.5 * (own_c[c, 1] + other_c[c, 1])
        effective = jnp.maximum(normal_pre - normal_hat, 0.0)
        growth = 0.5 * jnp.exp(state_value / fric_a)
        strength = effective * fric_a
        slip_speed = guess_ref[:, lanes]
        for _ in range(NEWTON):
            scaled = slip_speed * growth
            magnitude = jnp.abs(scaled)
            root = jnp.sqrt(1.0 + scaled * scaled)
            logged = jnp.log(magnitude + root)
            logged = jnp.where(scaled < 0.0, -logged, logged)
            mismatch = locked - 0.5 * imp_s * slip_speed - strength * logged
            slope_value = -0.5 * imp_s - strength * growth / root
            slip_speed = slip_speed - mismatch / slope_value
        shear_hat = locked - shear_pre - 0.5 * imp_s * slip_speed
        slot = lax.broadcasted_iota(jnp.int32, (points, LANES), 1) + c * LANES
        live = slot < count_ref[0]
        slip_ref[:, lanes] = jnp.where(live, slip_speed, 0.0)
        bound = jnp.where(live, par_ref[4, :, lanes] / (jnp.abs(slip_speed) + 1.0), FAR_BOUND)
        least = bound if least is None else jnp.minimum(least, bound)
        faced.append((normal_hat, shear_hat, live))
    bound = jnp.min(jnp.min(least, axis=0, keepdims=True), axis=1, keepdims=True)
    bound_out[...] = jnp.broadcast_to(bound, (1, LANES))

    def send_bound(hop):
        pltpu.make_async_remote_copy(
            src_ref=bound_out,
            dst_ref=bound_in.at[hop - 1],
            send_sem=bound_send,
            recv_sem=bound_recv,
            device_id=chip_at(hop),
            device_id_type=MESH,
        ).start()

    each_hop(send_bound)
    dip_over.start()
    start_if(False)
    turned = [jnp.transpose(pads[d])[0:deep] for d in range(3)]
    turned_wide = wide(jnp.concatenate(turned, axis=0), deep)
    for group in triples:
        multiply(turned_wide, lambda q: integ[q], keep_z(0), group)
    for group in triples:
        for q, fresh in zip(group, apply_star(0, group)):
            out_ref[q] = dofs_ref[q] + fresh
        fence()


    arrived(13)
    dip_over.wait_recv()
    fvals[...] = jnp.zeros(fvals.shape, F32)
    for lanes, (normal_hat, shear_hat, live) in zip(chunks, faced):
        hats = [normal_hat, shear_hat, 0.5 * (own_dip[:, lanes] + other_dip[:, lanes])]
        for k in range(3):
            impedance = par_ref[5 if k == 0 else 6, :, lanes]
            past = frame[k, 0:points, lanes]
            hats.append(frame[k + 3, 0:points, lanes] + orient * (hats[k] - past) / impedance)
        for q in range(quants):
            summed = None
            for k in range(6):
                term = fflux_ref[q, k : k + 1, lanes] * hats[k]
                summed = term if summed is None else summed + term
            fvals[q * rows : q * rows + points, lanes] = jnp.where(live, summed, 0.0)
    spread_pair = stacked(fvals[...])
    spread = lax.dot_general(
        spread_pair, fault_table[...], (((1,), (1,)), ((), ())), preferred_element_type=F32
    )
    half = spread.shape[0] // 2
    lifted[...] = spread[:half] + spread[half:]

    arrived(len(later))
    neighbour = jnp.concatenate([neigh_ref[f : f + 1, :] for f in range(faces)], axis=1)
    near_table = table(flat, neighbour)
    pick_all(near_table, local_part)
    lane_tile = lax.broadcasted_iota(jnp.int32, (faces, LANES), 1)
    wide_lane = lax.broadcasted_iota(jnp.int32, (basis, LANES), 1)
    duo_faces = range(0, faces, 2)

    def face_pairs(tile):
        shifted = pltpu.roll(jnp.concatenate([tile[1:], tile[:1]], axis=0), EDGE, 1)
        return jnp.where(lane_tile < EDGE, tile, shifted)

    paired = face_pairs(neigh_ref[...])
    far_keys = jnp.concatenate([paired[f : f + 1] for f in duo_faces], axis=1)
    far_table = table(blocks * block, far_keys, flat)
    for q in range(quants):
        for j in range(quants):
            pair_flux[q, j] = face_pairs(flux_ref[1, q, j])
    lift_pair = stacked(jnp.transpose(pads[3])[:deep])
    lift_wide = jnp.concatenate([lift_pair[:deep], lift_pair[deep:], lift_pair[:deep]], axis=1)
    for f in range(faces):
        columns = slice(f * elems, (f + 1) * elems)
        for q in range(quants):
            summed = lifted[q * rows : (q + 1) * rows, columns]
            for j in range(quants):
                inner = trace[j * rows : (j + 1) * rows, columns]
                near = local_part[j * rows : (j + 1) * rows, columns]
                summed = summed + flux_ref[0, q, j, f : f + 1, :] * inner
                summed = summed + flux_ref[1, q, j, f : f + 1, :] * near
            vals[q, f * face_rows : f * face_rows + rows] = summed

    def three(joined):
        high, low = split(joined)
        return jnp.concatenate([high, high, low], axis=0)

    for group in triples:
        result = dot(lift_wide, three(jnp.concatenate([vals[q] for q in group], axis=1)))
        for n, q in enumerate(group):
            out_ref[q] = out_ref[q] - result[:basis, n * elems : (n + 1) * elems]

    sorted_rows = jnp.concatenate(
        [pads[3, f * face_rows : (f + 1) * face_rows] for f in (*duo_faces, *range(1, faces, 2))],
        axis=0,
    )
    tall_lift = jnp.transpose(sorted_rows)[:deep]
    lift_lane = lax.broadcasted_iota(jnp.int32, (deep, LANES), 1)
    both_lifts = jnp.concatenate(
        [
            jnp.where(lift_lane < deep, tall_lift, 0.0),
            jnp.where(lift_lane < deep, pltpu.roll(tall_lift, LANES - deep, 1), 0.0),
        ],
        axis=0,
    )
    far_wide = wide(both_lifts, deep)

    for copy in copies:
        copy.wait_recv()
    columns = []
    for o in duos:
        upper, lower = halo_in[o], halo_in[o + 1]
        columns.append(
            jnp.concatenate(
                [
                    jnp.where(near_half, upper, pltpu.roll(lower, block, 1)),
                    jnp.where(near_half, pltpu.roll(upper, block, 1), lower),
                ],
                axis=0,
            )
        )
    far = pick(stacked(jnp.concatenate(columns, axis=1)), far_table)
    rest = jnp.zeros((face_rows - rows, LANES), F32)
    for group in triples:
        parts = []
        for q in group:
            pieces = []
            for c in range(len(duo_faces)):
                summed = None
                for j in range(quants):
                    term = pair_flux[q, j, 2 * c : 2 * c + 1, :] * far[
                        j * rows : (j + 1) * rows, c * LANES : (c + 1) * LANES
                    ]
                    summed = term if summed is None else summed + term
                pieces += [summed, rest]
            parts.append(jnp.concatenate(pieces, axis=0))
        result = dot(far_wide, three(jnp.concatenate(parts, axis=1)))
        for n, q in enumerate(group):
            even = result[:basis, n * elems : (n + 1) * elems]
            odd = result[deep : deep + basis, n * elems : (n + 1) * elems]
            both = even + pltpu.roll(odd, LANES - EDGE, 1)
            out_ref[q] = out_ref[q] - jnp.where(wide_lane < EDGE, both, 0.0)

    for copy in crossing:
        copy.wait_send()
    dip_over.wait_send()
    for copy in copies:
        copy.wait_send()
    best = bound_out[...]
    if chips > 1:
        pltpu.make_async_copy(bound_in, bound_in, bound_send).wait()
        pltpu.make_async_copy(bound_in, bound_in, bound_recv).wait()
        best = jnp.minimum(best, jnp.min(bound_in[...], axis=0))
    step_ref[...] = jnp.broadcast_to(best, step_ref.shape)


def store(dofs, slip, step, dofs_out, slip_out, step_out, least, sems):
    least[...] = step[0:1, 0:1]
    moves = ((dofs, dofs_out), (slip, slip_out), (least, step_out))
    copies = [pltpu.make_async_copy(a, b, sems.at[n]) for n, (a, b) in enumerate(moves)]
    for copy in copies:
        copy.start()
    for copy in copies:
        copy.wait()


def solution(mesh):
    chips, cores = mesh.shape["dom"], mesh.shape["fault"]
    hops = max(1, chips - 1)

    def on_device(
        modal_dofs,
        star_matrices,
        stiffness,
        face_proj,
        face_flux,
        neighbour_index,
        send_faces,
        fault_faces,
        fault_count,
        fault_params,
        slip_guess,
        fault_rotation,
        fault_flux,
    ):
        quants, basis, elems = modal_dofs.shape
        faces, _, points = face_proj.shape
        slots = fault_faces.shape[0]
        blocks = send_faces.shape[0]
        rows = up(points, 8)
        trace_rows = up(quants * rows, 32)
        star_matrices = jnp.transpose(star_matrices, (1, 2, 0, 3))
        face_proj = jnp.transpose(face_proj, (2, 0, 1))
        face_flux = jnp.transpose(face_flux, (0, 2, 3, 1, 4))
        fault_rotation = jnp.transpose(fault_rotation, (1, 0, 2))
        loaded = (
            modal_dofs,
            star_matrices,
            stiffness,
            face_proj,
            face_flux,
            neighbour_index,
            send_faces,
            fault_faces,
            fault_params,
            slip_guess,
            fault_rotation,
            fault_flux,
        )
        held = 4 * (quants * up(basis, 8) * elems + (rows + 8) * slots)
        vmem = pl.BlockSpec(memory_space=pltpu.VMEM)
        hbm = pl.BlockSpec(memory_space=pl.ANY)
        new_dofs, slip_rate, next_step = pl.pallas_call(
            functools.partial(kernel, chips, cores),
            out_shape=(
                pltpu.VMEM(modal_dofs.shape, F32),
                pltpu.VMEM(slip_guess.shape, F32),
                pltpu.VMEM((8, LANES), F32),
            ),
            in_specs=[hbm] * 13,
            out_specs=(vmem, vmem, vmem),
            scratch_shapes=[
                *(pltpu.VMEM(array.shape, array.dtype) for array in loaded),
                pltpu.SMEM(fault_count.shape, fault_count.dtype),
                pltpu.SemaphoreType.DMA((len(loaded) + fault_params.shape[0] + 1,)),
                pltpu.VMEM((quants, basis, elems), F32),
                pltpu.VMEM((2, 3, quants, basis, elems), F32),
                pltpu.VMEM((quants, basis, elems), F32),
                pltpu.VMEM((trace_rows, faces * elems), F32),
                pltpu.VMEM((4, LANES, LANES), F32),
                pltpu.VMEM((up(rows * faces, 8), LANES), F32),
                pltpu.VMEM((up(blocks, 8), LANES), jnp.int32),
                pltpu.VMEM((slots // LANES, 2, points, LANES), F32),
                pltpu.VMEM((slots // LANES, 2, points, LANES), F32),
                pltpu.VMEM((points, slots), F32),
                pltpu.VMEM((points, slots), F32),
                pltpu.VMEM((trace_rows, slots), F32),
                pltpu.VMEM((trace_rows, blocks // 2 * LANES), F32),
                pltpu.VMEM((trace_rows, faces * elems), F32),
                pltpu.VMEM((2 * (up(quants, 3) // 3) * up(3 * rows, 16), faces * elems), BF16),
                pltpu.VMEM((faces * elems, slots), BF16),
                pltpu.VMEM((faces * elems, blocks // 2 * LANES), BF16),
                pltpu.VMEM((6, rows, slots), F32),
                pltpu.VMEM((blocks, trace_rows // 2, LANES), F32),
                pltpu.VMEM((blocks, trace_rows // 2, LANES), F32),
                pltpu.VMEM((trace_rows, faces * elems), F32),
                pltpu.VMEM((trace_rows, slots), F32),
                pltpu.VMEM((quants, LANES, elems), F32),
                pltpu.VMEM((quants, quants, faces, elems), F32),
                pltpu.VMEM((1, LANES), F32),
                pltpu.VMEM((hops, 1, LANES), F32),
                pltpu.SemaphoreType.DMA((blocks,)),
                pltpu.SemaphoreType.DMA((blocks,)),
                pltpu.SemaphoreType.DMA((slots // LANES + 1,)),
                pltpu.SemaphoreType.DMA((slots // LANES + 1,)),
                pltpu.SemaphoreType.DMA,
                pltpu.SemaphoreType.DMA,
            ],
            compiler_params=pltpu.CompilerParams(
                collective_id=0, has_side_effects=True, vmem_limit_bytes=VMEM_BYTES - held
            ),
        )(
            modal_dofs,
            star_matrices,
            stiffness,
            face_proj,
            face_flux,
            neighbour_index,
            send_faces,
            fault_faces,
            fault_count,
            fault_params,
            slip_guess,
            fault_rotation,
            fault_flux,
        )
        results = (new_dofs, slip_rate, next_step)
        new_dofs, slip_rate, next_step = pl.pallas_call(
            store,
            out_shape=(
                jax.ShapeDtypeStruct(new_dofs.shape, F32),
                jax.ShapeDtypeStruct(slip_rate.shape, F32),
                jax.ShapeDtypeStruct((1, 1), F32),
            ),
            in_specs=[vmem] * len(results),
            out_specs=(hbm,) * len(results),
            scratch_shapes=[pltpu.VMEM((1, 1), F32), pltpu.SemaphoreType.DMA((len(results),))],
            compiler_params=pltpu.CompilerParams(vmem_limit_bytes=4 * 1024 * 1024),
        )(*results)
        return new_dofs, slip_rate, next_step.reshape(())

    return jax.shard_map(
        on_device,
        mesh=mesh,
        in_specs=(
            P(None, None, ("dom", "fault")),
            P(None, None, None, ("dom", "fault")),
            P(),
            P(),
            P(None, None, None, None, ("dom", "fault")),
            P(None, ("dom", "fault")),
            P(None, ("dom", "fault")),
            P(("dom", "fault")),
            P("dom"),
            P(None, None, "dom"),
            P(None, "dom"),
            P(None, None, "dom"),
            P(None, None, ("dom", "fault")),
        ),
        out_specs=(P(None, None, ("dom", "fault")), P(None, ("dom", "fault")), P()),
        check_vma=False,
    )
```

```python
import functools

import jax
import jax.numpy as jnp
from jax import lax
from jax.experimental import pallas as pl
from jax.experimental.pallas import tpu as pltpu
from jax.sharding import PartitionSpec as P

DERIVS = 6
NEWTON = 4
REACH = 8
DT_STEP = 0.15
FAR_BOUND = 1e30
LANES = 128
EDGE = 64
VMEM_BYTES = 67043328
MESH = pl.DeviceIdType.MESH
F32 = jnp.float32
BF16 = jnp.bfloat16


def up(size, unit):
    return -(-size // unit) * unit


def dot(left, right):
    return jnp.dot(left, right, preferred_element_type=F32)


def split(values):
    high = values.astype(BF16)
    low = (values - high.astype(F32)).astype(BF16)
    return high, low


def stacked(values):
    high, low = split(values)
    return jnp.concatenate([high, low], axis=0)


def pick(pair, table):
    half = pair.shape[0] // 2
    both = dot(pair, table)
    return both[:half] + both[half:]


def wide(matrix, width):
    high = matrix.astype(BF16).astype(F32)
    turned = high + pltpu.roll(matrix - high, width, 1)
    return jnp.concatenate([turned, high], axis=1)[:, : 3 * width].astype(BF16)


def kernel(
    chips,
    cores,
    dofs_hbm,
    star_hbm,
    stiff_hbm,
    proj_hbm,
    flux_hbm,
    neigh_hbm,
    send_hbm,
    faces_hbm,
    count_hbm,
    par_hbm,
    guess_hbm,
    rot_hbm,
    fflux_hbm,
    out_ref,
    slip_ref,
    step_ref,
    dofs_ref,
    star_ref,
    stiff_ref,
    proj_ref,
    flux_ref,
    neigh_ref,
    send_ref,
    faces_ref,
    par_ref,
    guess_ref,
    rot_ref,
    fflux_ref,
    count_ref,
    load_sem,
    x_buf,
    z_buf,
    integ,
    trace,
    pads,
    rows_buf,
    small,
    own_c,
    other_c,
    own_dip,
    other_dip,
    own_trace,
    chosen,
    local_part,
    trace_parts,
    fault_table,
    send_table,
    frame,
    halo_out,
    halo_in,
    lifted,
    fvals,
    vals,
    pair_flux,
    bound_out,
    bound_in,
    send_sem,
    recv_sem,
    fault_send,
    fault_recv,
    bound_send,
    bound_recv,
):
    quants, basis, elems = dofs_ref.shape
    points, faces, _ = proj_ref.shape
    slots = faces_ref.shape[0]
    blocks, block = send_ref.shape
    rows = up(points, 8)
    face_rows = LANES // faces
    deep = up(basis, 16)
    flat = faces * elems
    dom = lax.axis_index("dom")
    core = lax.axis_index("fault")
    total = chips * cores
    me = dom * cores + core
    shifts = (1, -1, REACH, -REACH)

    def device_at(shift):
        at = lax.rem(me + shift + total, total)
        return (at // cores, lax.rem(at, cores))

    def chip_at(shift):
        return (lax.rem(dom + shift, chips), core)

    partner = (dom, core + 1 - 2 * lax.rem(core, 2))

    def load(source, target):
        copy = pltpu.make_async_copy(source, target, load_sem.at[len(loads)])
        loads.append(copy)
        return copy

    loads = []
    first = [
        load(source, target)
        for source, target in (
            (stiff_hbm, stiff_ref),
            (proj_hbm, proj_ref),
            (dofs_hbm, dofs_ref),
            (star_hbm, star_ref),
        )
    ]
    later = [
        load(source, target)
        for source, target in (
            (faces_hbm, faces_ref),
            (send_hbm, send_ref),
            (rot_hbm, rot_ref),
            *((par_hbm.at[k], par_ref.at[k]) for k in (5, 6)),
            *((par_hbm.at[k], par_ref.at[k]) for k in range(5)),
            (guess_hbm, guess_ref),
            (count_hbm, count_ref),
            (fflux_hbm, fflux_ref),
            (neigh_hbm, neigh_ref),
            (flux_hbm.at[0], flux_ref.at[0]),
            (flux_hbm.at[1], flux_ref.at[1]),
        )
    ]
    for copy in first + later:
        copy.start()
    waiting = list(later)

    def fence():
        if waiting:
            waiting.pop(0).wait()

    def arrived(number):
        while len(later) - len(waiting) < number:
            fence()

    barrier = pltpu.get_barrier_semaphore()
    for shift in shifts:
        pl.semaphore_signal(barrier, inc=1, device_id=device_at(-shift), device_id_type=MESH)
    pl.semaphore_signal(barrier, inc=1, device_id=partner, device_id_type=MESH)

    def each_hop(step):
        if chips <= 32:
            for hop in range(1, chips):
                step(hop)
        else:
            lax.fori_loop(1, chips, lambda hop, carry: (step(hop), carry)[1], 0)

    def greet(hop):
        pl.semaphore_signal(barrier, inc=1, device_id=chip_at(hop), device_id_type=MESH)

    each_hop(greet)

    pads[...] = jnp.zeros(pads.shape, F32)
    rows_buf[...] = jnp.zeros(rows_buf.shape, F32)
    small[...] = jnp.zeros(small.shape, jnp.int32)
    vals[...] = jnp.zeros(vals.shape, F32)
    chosen[quants * rows :, :] = jnp.zeros((chosen.shape[0] - quants * rows, chosen.shape[1]), F32)
    first[0].wait()
    for d in range(3):
        pads[d, 0:basis, 0:basis] = stiff_ref[d]
    stiff_wide = wide(-jnp.concatenate([pads[d, 0:deep] for d in range(3)], axis=0), deep)

    gap = jnp.zeros((deep - basis, LANES), F32)
    triples = [tuple(range(q, min(q + 3, quants))) for q in range(0, quants, 3)]

    def tall(per_q, group):
        joined = jnp.concatenate(
            [jnp.concatenate([per_q(q), gap], axis=0) for q in group], axis=1
        )
        high, low = split(joined)
        return jnp.concatenate([high, high, low], axis=0)

    def multiply(matrix, per_q, keep, group):
        result = dot(matrix, tall(per_q, group))
        for n, q in enumerate(group):
            keep(q, result[:, n * elems : (n + 1) * elems])

    def keep_z(at):
        def keep(q, result):
            for d in range(3):
                z_buf[at, d, q] = result[d * deep : d * deep + basis]

        return keep

    def keep_trace(q, result):
        for f in range(faces):
            first_row = f * face_rows
            trace[q * rows : (q + 1) * rows, f * elems : (f + 1) * elems] = result[
                first_row : first_row + rows
            ]

    def apply_star(at, group):
        sums = [None] * len(group)
        for j in range(quants):
            for d in range(3):
                column = z_buf[at, d, j]
                for n, q in enumerate(group):
                    term = star_ref[q, j, d : d + 1, :] * column
                    sums[n] = term if sums[n] is None else sums[n] + term
        return sums

    first[2].wait()
    first[3].wait()
    for group in triples[:-1]:
        multiply(stiff_wide, lambda q: dofs_ref[q], keep_z(0), group)

    def table(height, wanted, base=0):
        keys = lax.broadcasted_iota(jnp.int16, (height, wanted.shape[1]), 0)
        match = keys == (wanted - base).astype(jnp.int16)
        return jnp.where(match, jnp.array(1.0, BF16), jnp.array(0.0, BF16))

    duos = range(0, blocks, 2)

    def build_tables():
        arrived(2)
        fault_table[...] = table(flat, faces_ref[...].reshape(1, slots))
        small[0:blocks, 0:block] = send_ref[...]
        behind = pltpu.roll(small[...], block, 1)
        wanted = jnp.concatenate(
            [small[o : o + 1] + behind[o + 1 : o + 2] for o in duos], axis=1
        )
        send_table[...] = table(flat, wanted)

    tier = trace_parts.shape[0] // (2 * len(triples))

    def split_trace(g):
        height = len(triples[g]) * rows
        base = triples[g][0] * rows
        spare = jnp.zeros((tier - height, flat), F32)
        both = stacked(jnp.concatenate([trace[base : base + height, :], spare], axis=0))
        trace_parts[2 * g * tier : 2 * (g + 1) * tier] = both

    def place(both, g, target):
        height = len(triples[g]) * rows
        base = triples[g][0] * rows
        target[base : base + height, :] = both[:height] + both[tier : tier + height]

    def pick_group(g, chosen_table, target):
        place(dot(trace_parts[2 * g * tier : 2 * (g + 1) * tier], chosen_table), g, target)

    def pick_all(chosen_table, target):
        both = dot(trace_parts[...], chosen_table)
        for g in range(len(triples)):
            place(both[2 * g * tier : 2 * (g + 1) * tier], g, target)

    def trace_matrix():
        first[1].wait()
        for p in range(points):
            rows_buf[p * faces : (p + 1) * faces, 0:basis] = proj_ref[p]
        for f in range(faces):
            pads[3, f * face_rows : f * face_rows + rows] = rows_buf[pl.ds(f, rows, faces), :]
        return wide(pads[3], deep)

    factor = DT_STEP
    for degree in range(1, DERIVS):
        at, then = (degree - 1) % 2, degree % 2
        past = factor
        factor = factor * DT_STEP / (degree + 1)
        last = degree == DERIVS - 1
        if last:
            build_tables()
            trace_wide = trace_matrix()
        for t, group in enumerate(triples):
            if t == 0:
                source = dofs_ref if degree == 1 else x_buf
                multiply(stiff_wide, lambda q: source[q], keep_z(at), triples[-1])
            elif last:
                multiply(trace_wide, lambda q: integ[q], keep_trace, triples[t - 1])
                if t > 1:
                    split_trace(t - 2)
            else:
                multiply(stiff_wide, lambda q: x_buf[q], keep_z(then), triples[t - 1])
            for q, fresh in zip(group, apply_star(at, group)):
                if not last:
                    x_buf[q] = fresh
                base = past * dofs_ref[q] if degree == 1 else integ[q]
                integ[q] = base + factor * fresh
            if t < len(triples) - 1:
                fence()
    multiply(trace_wide, lambda q: integ[q], keep_trace, triples[-1])
    split_trace(len(triples) - 2)
    split_trace(len(triples) - 1)
    pick_all(fault_table[...], own_trace)
    orient = jnp.where(core == 0, 1.0, -1.0).astype(F32)
    chunks = [slice(c * LANES, (c + 1) * LANES) for c in range(slots // LANES)]
    arrived(5)

    def turn(k, lanes):
        summed = None
        for j in range(quants):
            term = rot_ref[j, k : k + 1, lanes] * own_trace[j * rows : (j + 1) * rows, lanes]
            summed = term if summed is None else summed + term
        frame[k, :, lanes] = summed
        return summed[:points]

    def face_both(k, lanes):
        impedance = par_ref[5 if k == 0 else 6, :, lanes]
        stress, speed = turn(k, lanes), turn(k + 3, lanes)
        return stress - orient * impedance * speed

    def across(c):
        return pltpu.make_async_remote_copy(
            src_ref=own_c.at[c],
            dst_ref=other_c.at[c],
            send_sem=fault_send.at[c],
            recv_sem=fault_recv.at[c],
            device_id=partner,
            device_id_type=MESH,
        )

    crossing = [across(c) for c in range(len(chunks))]
    dip_over = pltpu.make_async_remote_copy(
        src_ref=own_dip,
        dst_ref=other_dip,
        send_sem=fault_send.at[len(chunks)],
        recv_sem=fault_recv.at[len(chunks)],
        device_id=partner,
        device_id_type=MESH,
    )
    for c, lanes in enumerate(chunks):
        for k in range(2):
            own_c[c, k] = face_both(k, lanes)
        if c == 0:
            pl.semaphore_wait(barrier, len(shifts) + chips)
        crossing[c].start()

    pick_all(send_table[...], chosen)
    half_rows = trace.shape[0] // 2
    lane = lax.broadcasted_iota(jnp.int32, (half_rows, LANES), 1)
    near_half = lane < block
    copies = []
    for o in duos:
        lanes = slice(o // 2 * LANES, (o // 2 + 1) * LANES)
        upper, lower = chosen[:half_rows, lanes], chosen[half_rows:, lanes]
        halo_out[o] = jnp.where(near_half, upper, pltpu.roll(lower, block, 1))
        halo_out[o + 1] = jnp.where(near_half, pltpu.roll(upper, block, 1), lower)
    for o, shift in enumerate(shifts):
        copies.append(
            pltpu.make_async_remote_copy(
                src_ref=halo_out.at[o],
                dst_ref=halo_in.at[o],
                send_sem=send_sem.at[o],
                recv_sem=recv_sem.at[o],
                device_id=device_at(shift),
                device_id_type=MESH,
            )
        )
    urgent = [lax.rem(me + shift + total, total) < cores for shift in shifts]

    def start_if(wanted):
        for copy, first_of_all in zip(copies, urgent):
            pl.when(first_of_all == wanted)(copy.start)

    start_if(True)
    for lanes in chunks:
        own_dip[:, lanes] = face_both(2, lanes)

    arrived(12)

    def slope_terms(slip_speed, growth):
        scaled = slip_speed * growth
        root = jnp.sqrt(1.0 + scaled * scaled)
        logged = jnp.log(jnp.abs(scaled) + root)
        return jnp.where(scaled < 0.0, -logged, logged), growth / root

    ready = []
    for lanes in chunks:
        growth = 0.5 * jnp.exp(par_ref[1, :, lanes] / par_ref[0, :, lanes])
        ready.append((growth, *slope_terms(guess_ref[:, lanes], growth)))
    least = None
    faced = []
    for c, lanes in enumerate(chunks):
        crossing[c].wait_recv()
        fric_a, normal_pre, shear_pre = (par_ref[k, :, lanes] for k in (0, 2, 3))
        imp_s = par_ref[6, :, lanes]
        normal_hat = 0.5 * (own_c[c, 0] + other_c[c, 0])
        locked = shear_pre + 0.5 * (own_c[c, 1] + other_c[c, 1])
        effective = jnp.maximum(normal_pre - normal_hat, 0.0)
        strength = effective * fric_a
        slip_speed = guess_ref[:, lanes]
        growth, logged, steepness = ready[c]
        for repeat in range(NEWTON):
            if repeat:
                logged, steepness = slope_terms(slip_speed, growth)
            mismatch = locked - 0.5 * imp_s * slip_speed - strength * logged
            slope_value = -0.5 * imp_s - strength * steepness
            slip_speed = slip_speed - mismatch / slope_value
        shear_hat = locked - shear_pre - 0.5 * imp_s * slip_speed
        slot = lax.broadcasted_iota(jnp.int32, (points, LANES), 1) + c * LANES
        live = slot < count_ref[0]
        slip_ref[:, lanes] = jnp.where(live, slip_speed, 0.0)
        bound = jnp.where(live, par_ref[4, :, lanes] / (jnp.abs(slip_speed) + 1.0), FAR_BOUND)
        least = bound if least is None else jnp.minimum(least, bound)
        faced.append((normal_hat, shear_hat, live))
    bound = jnp.min(jnp.min(least, axis=0, keepdims=True), axis=1, keepdims=True)
    bound_out[...] = jnp.broadcast_to(bound, (1, LANES))

    def send_bound(hop):
        pltpu.make_async_remote_copy(
            src_ref=bound_out,
            dst_ref=bound_in.at[hop - 1],
            send_sem=bound_send,
            recv_sem=bound_recv,
            device_id=chip_at(hop),
            device_id_type=MESH,
        ).start()

    each_hop(send_bound)
    dip_over.start()
    start_if(False)
    turned = [jnp.transpose(pads[d])[0:deep] for d in range(3)]
    turned_wide = wide(jnp.concatenate(turned, axis=0), deep)
    for group in triples:
        multiply(turned_wide, lambda q: integ[q], keep_z(0), group)
    for group in triples:
        for q, fresh in zip(group, apply_star(0, group)):
            out_ref[q] = dofs_ref[q] + fresh
        fence()


    arrived(13)
    dip_over.wait_recv()
    fvals[...] = jnp.zeros(fvals.shape, F32)
    for lanes, (normal_hat, shear_hat, live) in zip(chunks, faced):
        hats = [normal_hat, shear_hat, 0.5 * (own_dip[:, lanes] + other_dip[:, lanes])]
        for k in range(3):
            impedance = par_ref[5 if k == 0 else 6, :, lanes]
            past = frame[k, 0:points, lanes]
            hats.append(frame[k + 3, 0:points, lanes] + orient * (hats[k] - past) / impedance)
        for q in range(quants):
            summed = None
            for k in range(6):
                term = fflux_ref[q, k : k + 1, lanes] * hats[k]
                summed = term if summed is None else summed + term
            fvals[q * rows : q * rows + points, lanes] = jnp.where(live, summed, 0.0)
    spread_pair = stacked(fvals[...])
    spread = lax.dot_general(
        spread_pair, fault_table[...], (((1,), (1,)), ((), ())), preferred_element_type=F32
    )
    half = spread.shape[0] // 2
    lifted[...] = spread[:half] + spread[half:]

    arrived(len(later))
    neighbour = jnp.concatenate([neigh_ref[f : f + 1, :] for f in range(faces)], axis=1)
    near_table = table(flat, neighbour)
    pick_all(near_table, local_part)
    lane_tile = lax.broadcasted_iota(jnp.int32, (faces, LANES), 1)
    wide_lane = lax.broadcasted_iota(jnp.int32, (basis, LANES), 1)
    duo_faces = range(0, faces, 2)

    def face_pairs(tile):
        shifted = pltpu.roll(jnp.concatenate([tile[1:], tile[:1]], axis=0), EDGE, 1)
        return jnp.where(lane_tile < EDGE, tile, shifted)

    paired = face_pairs(neigh_ref[...])
    far_keys = jnp.concatenate([paired[f : f + 1] for f in duo_faces], axis=1)
    far_table = table(blocks * block, far_keys, flat)
    for q in range(quants):
        for j in range(quants):
            pair_flux[q, j] = face_pairs(flux_ref[1, q, j])
    lift_pair = stacked(jnp.transpose(pads[3])[:deep])
    lift_wide = jnp.concatenate([lift_pair[:deep], lift_pair[deep:], lift_pair[:deep]], axis=1)
    for f in range(faces):
        columns = slice(f * elems, (f + 1) * elems)
        for q in range(quants):
            summed = lifted[q * rows : (q + 1) * rows, columns]
            for j in range(quants):
                inner = trace[j * rows : (j + 1) * rows, columns]
                near = local_part[j * rows : (j + 1) * rows, columns]
                summed = summed + flux_ref[0, q, j, f : f + 1, :] * inner
                summed = summed + flux_ref[1, q, j, f : f + 1, :] * near
            vals[q, f * face_rows : f * face_rows + rows] = summed

    def three(joined):
        high, low = split(joined)
        return jnp.concatenate([high, high, low], axis=0)

    for group in triples:
        result = dot(lift_wide, three(jnp.concatenate([vals[q] for q in group], axis=1)))
        for n, q in enumerate(group):
            out_ref[q] = out_ref[q] - result[:basis, n * elems : (n + 1) * elems]

    sorted_rows = jnp.concatenate(
        [pads[3, f * face_rows : (f + 1) * face_rows] for f in (*duo_faces, *range(1, faces, 2))],
        axis=0,
    )
    tall_lift = jnp.transpose(sorted_rows)[:deep]
    lift_lane = lax.broadcasted_iota(jnp.int32, (deep, LANES), 1)
    both_lifts = jnp.concatenate(
        [
            jnp.where(lift_lane < deep, tall_lift, 0.0),
            jnp.where(lift_lane < deep, pltpu.roll(tall_lift, LANES - deep, 1), 0.0),
        ],
        axis=0,
    )
    far_wide = wide(both_lifts, deep)

    for copy in copies:
        copy.wait_recv()
    columns = []
    for o in duos:
        upper, lower = halo_in[o], halo_in[o + 1]
        columns.append(
            jnp.concatenate(
                [
                    jnp.where(near_half, upper, pltpu.roll(lower, block, 1)),
                    jnp.where(near_half, pltpu.roll(upper, block, 1), lower),
                ],
                axis=0,
            )
        )
    far = pick(stacked(jnp.concatenate(columns, axis=1)), far_table)
    rest = jnp.zeros((face_rows - rows, LANES), F32)
    for group in triples:
        parts = []
        for q in group:
            pieces = []
            for c in range(len(duo_faces)):
                summed = None
                for j in range(quants):
                    term = pair_flux[q, j, 2 * c : 2 * c + 1, :] * far[
                        j * rows : (j + 1) * rows, c * LANES : (c + 1) * LANES
                    ]
                    summed = term if summed is None else summed + term
                pieces += [summed, rest]
            parts.append(jnp.concatenate(pieces, axis=0))
        result = dot(far_wide, three(jnp.concatenate(parts, axis=1)))
        for n, q in enumerate(group):
            even = result[:basis, n * elems : (n + 1) * elems]
            odd = result[deep : deep + basis, n * elems : (n + 1) * elems]
            both = even + pltpu.roll(odd, LANES - EDGE, 1)
            out_ref[q] = out_ref[q] - jnp.where(wide_lane < EDGE, both, 0.0)

    for copy in crossing:
        copy.wait_send()
    dip_over.wait_send()
    for copy in copies:
        copy.wait_send()
    best = bound_out[...]
    if chips > 1:
        pltpu.make_async_copy(bound_in, bound_in, bound_send).wait()
        pltpu.make_async_copy(bound_in, bound_in, bound_recv).wait()
        best = jnp.minimum(best, jnp.min(bound_in[...], axis=0))
    step_ref[...] = jnp.broadcast_to(best, step_ref.shape)


def store(dofs, slip, step, dofs_out, slip_out, step_out, least, sems):
    least[...] = step[0:1, 0:1]
    moves = ((dofs, dofs_out), (slip, slip_out), (least, step_out))
    copies = [pltpu.make_async_copy(a, b, sems.at[n]) for n, (a, b) in enumerate(moves)]
    for copy in copies:
        copy.start()
    for copy in copies:
        copy.wait()


def solution(mesh):
    chips, cores = mesh.shape["dom"], mesh.shape["fault"]
    hops = max(1, chips - 1)

    def on_device(
        modal_dofs,
        star_matrices,
        stiffness,
        face_proj,
        face_flux,
        neighbour_index,
        send_faces,
        fault_faces,
        fault_count,
        fault_params,
        slip_guess,
        fault_rotation,
        fault_flux,
    ):
        quants, basis, elems = modal_dofs.shape
        faces, _, points = face_proj.shape
        slots = fault_faces.shape[0]
        blocks = send_faces.shape[0]
        rows = up(points, 8)
        trace_rows = up(quants * rows, 32)
        star_matrices = jnp.transpose(star_matrices, (1, 2, 0, 3))
        face_proj = jnp.transpose(face_proj, (2, 0, 1))
        face_flux = jnp.transpose(face_flux, (0, 2, 3, 1, 4))
        fault_rotation = jnp.transpose(fault_rotation, (1, 0, 2))
        loaded = (
            modal_dofs,
            star_matrices,
            stiffness,
            face_proj,
            face_flux,
            neighbour_index,
            send_faces,
            fault_faces,
            fault_params,
            slip_guess,
            fault_rotation,
            fault_flux,
        )
        held = 4 * (quants * up(basis, 8) * elems + (rows + 8) * slots)
        vmem = pl.BlockSpec(memory_space=pltpu.VMEM)
        hbm = pl.BlockSpec(memory_space=pl.ANY)
        new_dofs, slip_rate, next_step = pl.pallas_call(
            functools.partial(kernel, chips, cores),
            out_shape=(
                pltpu.VMEM(modal_dofs.shape, F32),
                pltpu.VMEM(slip_guess.shape, F32),
                pltpu.VMEM((8, LANES), F32),
            ),
            in_specs=[hbm] * 13,
            out_specs=(vmem, vmem, vmem),
            scratch_shapes=[
                *(pltpu.VMEM(array.shape, array.dtype) for array in loaded),
                pltpu.SMEM(fault_count.shape, fault_count.dtype),
                pltpu.SemaphoreType.DMA((len(loaded) + fault_params.shape[0] + 1,)),
                pltpu.VMEM((quants, basis, elems), F32),
                pltpu.VMEM((2, 3, quants, basis, elems), F32),
                pltpu.VMEM((quants, basis, elems), F32),
                pltpu.VMEM((trace_rows, faces * elems), F32),
                pltpu.VMEM((4, LANES, LANES), F32),
                pltpu.VMEM((up(rows * faces, 8), LANES), F32),
                pltpu.VMEM((up(blocks, 8), LANES), jnp.int32),
                pltpu.VMEM((slots // LANES, 2, points, LANES), F32),
                pltpu.VMEM((slots // LANES, 2, points, LANES), F32),
                pltpu.VMEM((points, slots), F32),
                pltpu.VMEM((points, slots), F32),
                pltpu.VMEM((trace_rows, slots), F32),
                pltpu.VMEM((trace_rows, blocks // 2 * LANES), F32),
                pltpu.VMEM((trace_rows, faces * elems), F32),
                pltpu.VMEM((2 * (up(quants, 3) // 3) * up(3 * rows, 16), faces * elems), BF16),
                pltpu.VMEM((faces * elems, slots), BF16),
                pltpu.VMEM((faces * elems, blocks // 2 * LANES), BF16),
                pltpu.VMEM((6, rows, slots), F32),
                pltpu.VMEM((blocks, trace_rows // 2, LANES), F32),
                pltpu.VMEM((blocks, trace_rows // 2, LANES), F32),
                pltpu.VMEM((trace_rows, faces * elems), F32),
                pltpu.VMEM((trace_rows, slots), F32),
                pltpu.VMEM((quants, LANES, elems), F32),
                pltpu.VMEM((quants, quants, faces, elems), F32),
                pltpu.VMEM((1, LANES), F32),
                pltpu.VMEM((hops, 1, LANES), F32),
                pltpu.SemaphoreType.DMA((blocks,)),
                pltpu.SemaphoreType.DMA((blocks,)),
                pltpu.SemaphoreType.DMA((slots // LANES + 1,)),
                pltpu.SemaphoreType.DMA((slots // LANES + 1,)),
                pltpu.SemaphoreType.DMA,
                pltpu.SemaphoreType.DMA,
            ],
            compiler_params=pltpu.CompilerParams(
                collective_id=0, has_side_effects=True, vmem_limit_bytes=VMEM_BYTES - held
            ),
        )(
            modal_dofs,
            star_matrices,
            stiffness,
            face_proj,
            face_flux,
            neighbour_index,
            send_faces,
            fault_faces,
            fault_count,
            fault_params,
            slip_guess,
            fault_rotation,
            fault_flux,
        )
        results = (new_dofs, slip_rate, next_step)
        new_dofs, slip_rate, next_step = pl.pallas_call(
            store,
            out_shape=(
                jax.ShapeDtypeStruct(new_dofs.shape, F32),
                jax.ShapeDtypeStruct(slip_rate.shape, F32),
                jax.ShapeDtypeStruct((1, 1), F32),
            ),
            in_specs=[vmem] * len(results),
            out_specs=(hbm,) * len(results),
            scratch_shapes=[pltpu.VMEM((1, 1), F32), pltpu.SemaphoreType.DMA((len(results),))],
            compiler_params=pltpu.CompilerParams(vmem_limit_bytes=4 * 1024 * 1024),
        )(*results)
        return new_dofs, slip_rate, next_step.reshape(())

    return jax.shard_map(
        on_device,
        mesh=mesh,
        in_specs=(
            P(None, None, ("dom", "fault")),
            P(None, None, None, ("dom", "fault")),
            P(),
            P(),
            P(None, None, None, None, ("dom", "fault")),
            P(None, ("dom", "fault")),
            P(None, ("dom", "fault")),
            P(("dom", "fault")),
            P("dom"),
            P(None, None, "dom"),
            P(None, "dom"),
            P(None, None, "dom"),
            P(None, None, ("dom", "fault")),
        ),
        out_specs=(P(None, None, ("dom", "fault")), P(None, ("dom", "fault")), P()),
        check_vma=False,
    )
```

```python
import functools

import jax
import jax.numpy as jnp
from jax import lax
from jax.experimental import pallas as pl
from jax.experimental.pallas import tpu as pltpu
from jax.sharding import PartitionSpec as P

DERIVS = 6
NEWTON = 4
REACH = 8
DT_STEP = 0.15
FAR_BOUND = 1e30
LANES = 128
EDGE = 64
VMEM_BYTES = 67043328
MESH = pl.DeviceIdType.MESH
F32 = jnp.float32
BF16 = jnp.bfloat16


def up(size, unit):
    return -(-size // unit) * unit


def dot(left, right):
    return jnp.dot(left, right, preferred_element_type=F32)


def split(values):
    high = values.astype(BF16)
    low = (values - high.astype(F32)).astype(BF16)
    return high, low


def stacked(values):
    high, low = split(values)
    return jnp.concatenate([high, low], axis=0)


def pick(pair, table):
    half = pair.shape[0] // 2
    both = dot(pair, table)
    return both[:half] + both[half:]


def wide(matrix, width):
    high = matrix.astype(BF16).astype(F32)
    turned = high + pltpu.roll(matrix - high, width, 1)
    return jnp.concatenate([turned, high], axis=1)[:, : 3 * width].astype(BF16)


def kernel(
    chips,
    cores,
    dofs_hbm,
    star_hbm,
    stiff_hbm,
    proj_hbm,
    flux_hbm,
    neigh_hbm,
    send_hbm,
    faces_hbm,
    count_hbm,
    par_hbm,
    guess_hbm,
    rot_hbm,
    fflux_hbm,
    out_ref,
    slip_ref,
    step_ref,
    dofs_ref,
    star_ref,
    stiff_ref,
    proj_ref,
    flux_ref,
    neigh_ref,
    send_ref,
    faces_ref,
    par_ref,
    guess_ref,
    rot_ref,
    fflux_ref,
    count_ref,
    load_sem,
    x_buf,
    z_buf,
    integ,
    trace,
    pads,
    rows_buf,
    small,
    own_c,
    other_c,
    own_dip,
    other_dip,
    own_trace,
    chosen,
    local_part,
    trace_parts,
    fault_table,
    send_table,
    frame,
    halo_out,
    halo_in,
    lifted,
    fvals,
    vals,
    pair_flux,
    bound_out,
    bound_in,
    send_sem,
    recv_sem,
    fault_send,
    fault_recv,
    bound_send,
    bound_recv,
):
    quants, basis, elems = dofs_ref.shape
    points, faces, _ = proj_ref.shape
    slots = faces_ref.shape[0]
    blocks, block = send_ref.shape
    rows = up(points, 8)
    face_rows = LANES // faces
    deep = up(basis, 16)
    flat = faces * elems
    dom = lax.axis_index("dom")
    core = lax.axis_index("fault")
    total = chips * cores
    me = dom * cores + core
    shifts = (1, -1, REACH, -REACH)

    def device_at(shift):
        at = lax.rem(me + shift + total, total)
        return (at // cores, lax.rem(at, cores))

    def chip_at(shift):
        return (lax.rem(dom + shift, chips), core)

    partner = (dom, core + 1 - 2 * lax.rem(core, 2))

    def load(source, target):
        copy = pltpu.make_async_copy(source, target, load_sem.at[len(loads)])
        loads.append(copy)
        return copy

    loads = []
    first = [
        load(source, target)
        for source, target in (
            (stiff_hbm, stiff_ref),
            (proj_hbm, proj_ref),
            (dofs_hbm, dofs_ref),
            (star_hbm, star_ref),
        )
    ]
    later = [
        load(source, target)
        for source, target in (
            (faces_hbm, faces_ref),
            (send_hbm, send_ref),
            (rot_hbm, rot_ref),
            *((par_hbm.at[k], par_ref.at[k]) for k in (5, 6)),
            *((par_hbm.at[k], par_ref.at[k]) for k in range(5)),
            (guess_hbm, guess_ref),
            (count_hbm, count_ref),
            (fflux_hbm, fflux_ref),
            (neigh_hbm, neigh_ref),
            (flux_hbm.at[0], flux_ref.at[0]),
            (flux_hbm.at[1], flux_ref.at[1]),
        )
    ]
    for copy in first + later:
        copy.start()
    waiting = list(later)

    def fence():
        if waiting:
            waiting.pop(0).wait()

    def arrived(number):
        while len(later) - len(waiting) < number:
            fence()

    barrier = pltpu.get_barrier_semaphore()
    for shift in shifts:
        pl.semaphore_signal(barrier, inc=1, device_id=device_at(-shift), device_id_type=MESH)
    pl.semaphore_signal(barrier, inc=1, device_id=partner, device_id_type=MESH)

    def each_hop(step):
        if chips <= 32:
            for hop in range(1, chips):
                step(hop)
        else:
            lax.fori_loop(1, chips, lambda hop, carry: (step(hop), carry)[1], 0)

    def greet(hop):
        pl.semaphore_signal(barrier, inc=1, device_id=chip_at(hop), device_id_type=MESH)

    each_hop(greet)

    pads[...] = jnp.zeros(pads.shape, F32)
    rows_buf[...] = jnp.zeros(rows_buf.shape, F32)
    small[...] = jnp.zeros(small.shape, jnp.int32)
    vals[...] = jnp.zeros(vals.shape, F32)
    chosen[quants * rows :, :] = jnp.zeros((chosen.shape[0] - quants * rows, chosen.shape[1]), F32)
    first[0].wait()
    for d in range(3):
        pads[d, 0:basis, 0:basis] = stiff_ref[d]
    stiff_wide = wide(-jnp.concatenate([pads[d, 0:deep] for d in range(3)], axis=0), deep)

    gap = jnp.zeros((deep - basis, LANES), F32)
    triples = [tuple(range(q, min(q + 3, quants))) for q in range(0, quants, 3)]

    def tall(per_q, group):
        joined = jnp.concatenate(
            [jnp.concatenate([per_q(q), gap], axis=0) for q in group], axis=1
        )
        high, low = split(joined)
        return jnp.concatenate([high, high, low], axis=0)

    def multiply(matrix, per_q, keep, group):
        result = dot(matrix, tall(per_q, group))
        for n, q in enumerate(group):
            keep(q, result[:, n * elems : (n + 1) * elems])

    def keep_z(at):
        def keep(q, result):
            for d in range(3):
                z_buf[at, d, q] = result[d * deep : d * deep + basis]

        return keep

    def keep_trace(q, result):
        for f in range(faces):
            first_row = f * face_rows
            trace[q * rows : (q + 1) * rows, f * elems : (f + 1) * elems] = result[
                first_row : first_row + rows
            ]

    def apply_star(at, group):
        sums = [None] * len(group)
        for j in range(quants):
            for d in range(3):
                column = z_buf[at, d, j]
                for n, q in enumerate(group):
                    term = star_ref[q, j, d : d + 1, :] * column
                    sums[n] = term if sums[n] is None else sums[n] + term
        return sums

    first[2].wait()
    first[3].wait()
    for group in triples[:-1]:
        multiply(stiff_wide, lambda q: dofs_ref[q], keep_z(0), group)

    def table(height, wanted, base=0):
        keys = lax.broadcasted_iota(jnp.int16, (height, wanted.shape[1]), 0)
        match = keys == (wanted - base).astype(jnp.int16)
        return jnp.where(match, jnp.array(1.0, BF16), jnp.array(0.0, BF16))

    duos = range(0, blocks, 2)

    def build_tables():
        arrived(2)
        fault_table[...] = table(flat, faces_ref[...].reshape(1, slots))
        small[0:blocks, 0:block] = send_ref[...]
        behind = pltpu.roll(small[...], block, 1)
        wanted = jnp.concatenate(
            [small[o : o + 1] + behind[o + 1 : o + 2] for o in duos], axis=1
        )
        send_table[...] = table(flat, wanted)

    tier = trace_parts.shape[0] // (2 * len(triples))

    def split_trace(g):
        height = len(triples[g]) * rows
        base = triples[g][0] * rows
        spare = jnp.zeros((tier - height, flat), F32)
        both = stacked(jnp.concatenate([trace[base : base + height, :], spare], axis=0))
        trace_parts[2 * g * tier : 2 * (g + 1) * tier] = both

    def place(both, g, target):
        height = len(triples[g]) * rows
        base = triples[g][0] * rows
        target[base : base + height, :] = both[:height] + both[tier : tier + height]

    def pick_group(g, chosen_table, target):
        place(dot(trace_parts[2 * g * tier : 2 * (g + 1) * tier], chosen_table), g, target)

    def pick_all(chosen_table, target):
        both = dot(trace_parts[...], chosen_table)
        for g in range(len(triples)):
            place(both[2 * g * tier : 2 * (g + 1) * tier], g, target)

    def trace_matrix():
        first[1].wait()
        for p in range(points):
            rows_buf[p * faces : (p + 1) * faces, 0:basis] = proj_ref[p]
        for f in range(faces):
            pads[3, f * face_rows : f * face_rows + rows] = rows_buf[pl.ds(f, rows, faces), :]
        return wide(pads[3], deep)

    factor = DT_STEP
    for degree in range(1, DERIVS):
        at, then = (degree - 1) % 2, degree % 2
        past = factor
        factor = factor * DT_STEP / (degree + 1)
        last = degree == DERIVS - 1
        if last:
            build_tables()
            trace_wide = trace_matrix()
        for t, group in enumerate(triples):
            if t == 0:
                source = dofs_ref if degree == 1 else x_buf
                multiply(stiff_wide, lambda q: source[q], keep_z(at), triples[-1])
            elif last:
                multiply(trace_wide, lambda q: integ[q], keep_trace, triples[t - 1])
                if t > 1:
                    split_trace(t - 2)
            else:
                multiply(stiff_wide, lambda q: x_buf[q], keep_z(then), triples[t - 1])
            for q, fresh in zip(group, apply_star(at, group)):
                if not last:
                    x_buf[q] = fresh
                base = past * dofs_ref[q] if degree == 1 else integ[q]
                integ[q] = base + factor * fresh
            if t < len(triples) - 1 and not (last and t == 1):
                fence()
    multiply(trace_wide, lambda q: integ[q], keep_trace, triples[-1])
    split_trace(len(triples) - 2)
    split_trace(len(triples) - 1)
    pick_all(fault_table[...], own_trace)
    orient = jnp.where(core == 0, 1.0, -1.0).astype(F32)
    chunks = [slice(c * LANES, (c + 1) * LANES) for c in range(slots // LANES)]
    arrived(5)

    def turn(k, lanes):
        summed = None
        for j in range(quants):
            term = rot_ref[j, k : k + 1, lanes] * own_trace[j * rows : (j + 1) * rows, lanes]
            summed = term if summed is None else summed + term
        frame[k, :, lanes] = summed
        return summed[:points]

    def face_both(k, lanes):
        impedance = par_ref[5 if k == 0 else 6, :, lanes]
        stress, speed = turn(k, lanes), turn(k + 3, lanes)
        return stress - orient * impedance * speed

    def across(c):
        return pltpu.make_async_remote_copy(
            src_ref=own_c.at[c],
            dst_ref=other_c.at[c],
            send_sem=fault_send.at[c],
            recv_sem=fault_recv.at[c],
            device_id=partner,
            device_id_type=MESH,
        )

    crossing = [across(c) for c in range(len(chunks))]
    dip_over = pltpu.make_async_remote_copy(
        src_ref=own_dip,
        dst_ref=other_dip,
        send_sem=fault_send.at[len(chunks)],
        recv_sem=fault_recv.at[len(chunks)],
        device_id=partner,
        device_id_type=MESH,
    )
    for c, lanes in enumerate(chunks):
        for k in range(2):
            own_c[c, k] = face_both(k, lanes)
        if c == 0:
            pl.semaphore_wait(barrier, len(shifts) + chips)
        crossing[c].start()

    pick_all(send_table[...], chosen)
    half_rows = trace.shape[0] // 2
    lane = lax.broadcasted_iota(jnp.int32, (half_rows, LANES), 1)
    near_half = lane < block
    copies = []
    for o in duos:
        lanes = slice(o // 2 * LANES, (o // 2 + 1) * LANES)
        upper, lower = chosen[:half_rows, lanes], chosen[half_rows:, lanes]
        halo_out[o] = jnp.where(near_half, upper, pltpu.roll(lower, block, 1))
        halo_out[o + 1] = jnp.where(near_half, pltpu.roll(upper, block, 1), lower)
    for o, shift in enumerate(shifts):
        copies.append(
            pltpu.make_async_remote_copy(
                src_ref=halo_out.at[o],
                dst_ref=halo_in.at[o],
                send_sem=send_sem.at[o],
                recv_sem=recv_sem.at[o],
                device_id=device_at(shift),
                device_id_type=MESH,
            )
        )
    urgent = [lax.rem(me + shift + total, total) < cores for shift in shifts]

    def start_if(wanted):
        for copy, first_of_all in zip(copies, urgent):
            pl.when(first_of_all == wanted)(copy.start)

    start_if(True)
    for lanes in chunks:
        own_dip[:, lanes] = face_both(2, lanes)

    arrived(12)

    def slope_terms(slip_speed, growth):
        scaled = slip_speed * growth
        root = jnp.sqrt(1.0 + scaled * scaled)
        logged = jnp.log(jnp.abs(scaled) + root)
        return jnp.where(scaled < 0.0, -logged, logged), growth / root

    ready = []
    for lanes in chunks:
        growth = 0.5 * jnp.exp(par_ref[1, :, lanes] / par_ref[0, :, lanes])
        ready.append((growth, *slope_terms(guess_ref[:, lanes], growth)))
    least = None
    faced = []
    for c, lanes in enumerate(chunks):
        crossing[c].wait_recv()
        fric_a, normal_pre, shear_pre = (par_ref[k, :, lanes] for k in (0, 2, 3))
        imp_s = par_ref[6, :, lanes]
        normal_hat = 0.5 * (own_c[c, 0] + other_c[c, 0])
        locked = shear_pre + 0.5 * (own_c[c, 1] + other_c[c, 1])
        effective = jnp.maximum(normal_pre - normal_hat, 0.0)
        strength = effective * fric_a
        slip_speed = guess_ref[:, lanes]
        growth, logged, steepness = ready[c]
        for repeat in range(NEWTON):
            if repeat:
                logged, steepness = slope_terms(slip_speed, growth)
            mismatch = locked - 0.5 * imp_s * slip_speed - strength * logged
            slope_value = -0.5 * imp_s - strength * steepness
            slip_speed = slip_speed - mismatch / slope_value
        shear_hat = locked - shear_pre - 0.5 * imp_s * slip_speed
        slot = lax.broadcasted_iota(jnp.int32, (points, LANES), 1) + c * LANES
        live = slot < count_ref[0]
        slip_ref[:, lanes] = jnp.where(live, slip_speed, 0.0)
        bound = jnp.where(live, par_ref[4, :, lanes] / (jnp.abs(slip_speed) + 1.0), FAR_BOUND)
        least = bound if least is None else jnp.minimum(least, bound)
        faced.append((normal_hat, shear_hat, live))
    bound = jnp.min(jnp.min(least, axis=0, keepdims=True), axis=1, keepdims=True)
    bound_out[...] = jnp.broadcast_to(bound, (1, LANES))

    def send_bound(hop):
        pltpu.make_async_remote_copy(
            src_ref=bound_out,
            dst_ref=bound_in.at[hop - 1],
            send_sem=bound_send,
            recv_sem=bound_recv,
            device_id=chip_at(hop),
            device_id_type=MESH,
        ).start()

    each_hop(send_bound)
    dip_over.start()
    start_if(False)
    turned = [jnp.transpose(pads[d])[0:deep] for d in range(3)]
    turned_wide = wide(jnp.concatenate(turned, axis=0), deep)
    for group in triples:
        multiply(turned_wide, lambda q: integ[q], keep_z(0), group)
    for group in triples:
        for q, fresh in zip(group, apply_star(0, group)):
            out_ref[q] = dofs_ref[q] + fresh
        fence()


    arrived(13)
    dip_over.wait_recv()
    fvals[...] = jnp.zeros(fvals.shape, F32)
    for lanes, (normal_hat, shear_hat, live) in zip(chunks, faced):
        hats = [normal_hat, shear_hat, 0.5 * (own_dip[:, lanes] + other_dip[:, lanes])]
        for k in range(3):
            impedance = par_ref[5 if k == 0 else 6, :, lanes]
            past = frame[k, 0:points, lanes]
            hats.append(frame[k + 3, 0:points, lanes] + orient * (hats[k] - past) / impedance)
        for q in range(quants):
            summed = None
            for k in range(6):
                term = fflux_ref[q, k : k + 1, lanes] * hats[k]
                summed = term if summed is None else summed + term
            fvals[q * rows : q * rows + points, lanes] = jnp.where(live, summed, 0.0)
    spread_pair = stacked(fvals[...])
    spread = lax.dot_general(
        spread_pair, fault_table[...], (((1,), (1,)), ((), ())), preferred_element_type=F32
    )
    half = spread.shape[0] // 2
    lifted[...] = spread[:half] + spread[half:]

    arrived(len(later))
    neighbour = jnp.concatenate([neigh_ref[f : f + 1, :] for f in range(faces)], axis=1)
    near_table = table(flat, neighbour)
    pick_all(near_table, local_part)
    lane_tile = lax.broadcasted_iota(jnp.int32, (faces, LANES), 1)
    wide_lane = lax.broadcasted_iota(jnp.int32, (basis, LANES), 1)
    duo_faces = range(0, faces, 2)

    def face_pairs(tile):
        shifted = pltpu.roll(jnp.concatenate([tile[1:], tile[:1]], axis=0), EDGE, 1)
        return jnp.where(lane_tile < EDGE, tile, shifted)

    paired = face_pairs(neigh_ref[...])
    far_keys = jnp.concatenate([paired[f : f + 1] for f in duo_faces], axis=1)
    far_table = table(blocks * block, far_keys, flat)
    for q in range(quants):
        for j in range(quants):
            pair_flux[q, j] = face_pairs(flux_ref[1, q, j])
    lift_pair = stacked(jnp.transpose(pads[3])[:deep])
    lift_wide = jnp.concatenate([lift_pair[:deep], lift_pair[deep:], lift_pair[:deep]], axis=1)
    for f in range(faces):
        columns = slice(f * elems, (f + 1) * elems)
        for q in range(quants):
            summed = lifted[q * rows : (q + 1) * rows, columns]
            for j in range(quants):
                inner = trace[j * rows : (j + 1) * rows, columns]
                near = local_part[j * rows : (j + 1) * rows, columns]
                summed = summed + flux_ref[0, q, j, f : f + 1, :] * inner
                summed = summed + flux_ref[1, q, j, f : f + 1, :] * near
            vals[q, f * face_rows : f * face_rows + rows] = summed

    def three(joined):
        high, low = split(joined)
        return jnp.concatenate([high, high, low], axis=0)

    for group in triples:
        result = dot(lift_wide, three(jnp.concatenate([vals[q] for q in group], axis=1)))
        for n, q in enumerate(group):
            out_ref[q] = out_ref[q] - result[:basis, n * elems : (n + 1) * elems]

    sorted_rows = jnp.concatenate(
        [pads[3, f * face_rows : (f + 1) * face_rows] for f in (*duo_faces, *range(1, faces, 2))],
        axis=0,
    )
    tall_lift = jnp.transpose(sorted_rows)[:deep]
    lift_lane = lax.broadcasted_iota(jnp.int32, (deep, LANES), 1)
    both_lifts = jnp.concatenate(
        [
            jnp.where(lift_lane < deep, tall_lift, 0.0),
            jnp.where(lift_lane < deep, pltpu.roll(tall_lift, LANES - deep, 1), 0.0),
        ],
        axis=0,
    )
    far_wide = wide(both_lifts, deep)

    for copy in copies:
        copy.wait_recv()
    columns = []
    for o in duos:
        upper, lower = halo_in[o], halo_in[o + 1]
        columns.append(
            jnp.concatenate(
                [
                    jnp.where(near_half, upper, pltpu.roll(lower, block, 1)),
                    jnp.where(near_half, pltpu.roll(upper, block, 1), lower),
                ],
                axis=0,
            )
        )
    far = pick(stacked(jnp.concatenate(columns, axis=1)), far_table)
    rest = jnp.zeros((face_rows - rows, LANES), F32)
    for group in triples:
        parts = []
        for q in group:
            pieces = []
            for c in range(len(duo_faces)):
                summed = None
                for j in range(quants):
                    term = pair_flux[q, j, 2 * c : 2 * c + 1, :] * far[
                        j * rows : (j + 1) * rows, c * LANES : (c + 1) * LANES
                    ]
                    summed = term if summed is None else summed + term
                pieces += [summed, rest]
            parts.append(jnp.concatenate(pieces, axis=0))
        result = dot(far_wide, three(jnp.concatenate(parts, axis=1)))
        for n, q in enumerate(group):
            even = result[:basis, n * elems : (n + 1) * elems]
            odd = result[deep : deep + basis, n * elems : (n + 1) * elems]
            both = even + pltpu.roll(odd, LANES - EDGE, 1)
            out_ref[q] = out_ref[q] - jnp.where(wide_lane < EDGE, both, 0.0)

    for copy in crossing:
        copy.wait_send()
    dip_over.wait_send()
    for copy in copies:
        copy.wait_send()
    best = bound_out[...]
    if chips > 1:
        pltpu.make_async_copy(bound_in, bound_in, bound_send).wait()
        pltpu.make_async_copy(bound_in, bound_in, bound_recv).wait()
        best = jnp.minimum(best, jnp.min(bound_in[...], axis=0))
    step_ref[...] = jnp.broadcast_to(best, step_ref.shape)


def store(dofs, slip, step, dofs_out, slip_out, step_out, least, sems):
    least[...] = step[0:1, 0:1]
    moves = ((dofs, dofs_out), (slip, slip_out), (least, step_out))
    copies = [pltpu.make_async_copy(a, b, sems.at[n]) for n, (a, b) in enumerate(moves)]
    for copy in copies:
        copy.start()
    for copy in copies:
        copy.wait()


def solution(mesh):
    chips, cores = mesh.shape["dom"], mesh.shape["fault"]
    hops = max(1, chips - 1)

    def on_device(
        modal_dofs,
        star_matrices,
        stiffness,
        face_proj,
        face_flux,
        neighbour_index,
        send_faces,
        fault_faces,
        fault_count,
        fault_params,
        slip_guess,
        fault_rotation,
        fault_flux,
    ):
        quants, basis, elems = modal_dofs.shape
        faces, _, points = face_proj.shape
        slots = fault_faces.shape[0]
        blocks = send_faces.shape[0]
        rows = up(points, 8)
        trace_rows = up(quants * rows, 32)
        star_matrices = jnp.transpose(star_matrices, (1, 2, 0, 3))
        face_proj = jnp.transpose(face_proj, (2, 0, 1))
        face_flux = jnp.transpose(face_flux, (0, 2, 3, 1, 4))
        fault_rotation = jnp.transpose(fault_rotation, (1, 0, 2))
        loaded = (
            modal_dofs,
            star_matrices,
            stiffness,
            face_proj,
            face_flux,
            neighbour_index,
            send_faces,
            fault_faces,
            fault_params,
            slip_guess,
            fault_rotation,
            fault_flux,
        )
        held = 4 * (quants * up(basis, 8) * elems + (rows + 8) * slots)
        vmem = pl.BlockSpec(memory_space=pltpu.VMEM)
        hbm = pl.BlockSpec(memory_space=pl.ANY)
        new_dofs, slip_rate, next_step = pl.pallas_call(
            functools.partial(kernel, chips, cores),
            out_shape=(
                pltpu.VMEM(modal_dofs.shape, F32),
                pltpu.VMEM(slip_guess.shape, F32),
                pltpu.VMEM((8, LANES), F32),
            ),
            in_specs=[hbm] * 13,
            out_specs=(vmem, vmem, vmem),
            scratch_shapes=[
                *(pltpu.VMEM(array.shape, array.dtype) for array in loaded),
                pltpu.SMEM(fault_count.shape, fault_count.dtype),
                pltpu.SemaphoreType.DMA((len(loaded) + fault_params.shape[0] + 1,)),
                pltpu.VMEM((quants, basis, elems), F32),
                pltpu.VMEM((2, 3, quants, basis, elems), F32),
                pltpu.VMEM((quants, basis, elems), F32),
                pltpu.VMEM((trace_rows, faces * elems), F32),
                pltpu.VMEM((4, LANES, LANES), F32),
                pltpu.VMEM((up(rows * faces, 8), LANES), F32),
                pltpu.VMEM((up(blocks, 8), LANES), jnp.int32),
                pltpu.VMEM((slots // LANES, 2, points, LANES), F32),
                pltpu.VMEM((slots // LANES, 2, points, LANES), F32),
                pltpu.VMEM((points, slots), F32),
                pltpu.VMEM((points, slots), F32),
                pltpu.VMEM((trace_rows, slots), F32),
                pltpu.VMEM((trace_rows, blocks // 2 * LANES), F32),
                pltpu.VMEM((trace_rows, faces * elems), F32),
                pltpu.VMEM((2 * (up(quants, 3) // 3) * up(3 * rows, 16), faces * elems), BF16),
                pltpu.VMEM((faces * elems, slots), BF16),
                pltpu.VMEM((faces * elems, blocks // 2 * LANES), BF16),
                pltpu.VMEM((6, rows, slots), F32),
                pltpu.VMEM((blocks, trace_rows // 2, LANES), F32),
                pltpu.VMEM((blocks, trace_rows // 2, LANES), F32),
                pltpu.VMEM((trace_rows, faces * elems), F32),
                pltpu.VMEM((trace_rows, slots), F32),
                pltpu.VMEM((quants, LANES, elems), F32),
                pltpu.VMEM((quants, quants, faces, elems), F32),
                pltpu.VMEM((1, LANES), F32),
                pltpu.VMEM((hops, 1, LANES), F32),
                pltpu.SemaphoreType.DMA((blocks,)),
                pltpu.SemaphoreType.DMA((blocks,)),
                pltpu.SemaphoreType.DMA((slots // LANES + 1,)),
                pltpu.SemaphoreType.DMA((slots // LANES + 1,)),
                pltpu.SemaphoreType.DMA,
                pltpu.SemaphoreType.DMA,
            ],
            compiler_params=pltpu.CompilerParams(
                collective_id=0, has_side_effects=True, vmem_limit_bytes=VMEM_BYTES - held
            ),
        )(
            modal_dofs,
            star_matrices,
            stiffness,
            face_proj,
            face_flux,
            neighbour_index,
            send_faces,
            fault_faces,
            fault_count,
            fault_params,
            slip_guess,
            fault_rotation,
            fault_flux,
        )
        results = (new_dofs, slip_rate, next_step)
        new_dofs, slip_rate, next_step = pl.pallas_call(
            store,
            out_shape=(
                jax.ShapeDtypeStruct(new_dofs.shape, F32),
                jax.ShapeDtypeStruct(slip_rate.shape, F32),
                jax.ShapeDtypeStruct((1, 1), F32),
            ),
            in_specs=[vmem] * len(results),
            out_specs=(hbm,) * len(results),
            scratch_shapes=[pltpu.VMEM((1, 1), F32), pltpu.SemaphoreType.DMA((len(results),))],
            compiler_params=pltpu.CompilerParams(vmem_limit_bytes=4 * 1024 * 1024),
        )(*results)
        return new_dofs, slip_rate, next_step.reshape(())

    return jax.shard_map(
        on_device,
        mesh=mesh,
        in_specs=(
            P(None, None, ("dom", "fault")),
            P(None, None, None, ("dom", "fault")),
            P(),
            P(),
            P(None, None, None, None, ("dom", "fault")),
            P(None, ("dom", "fault")),
            P(None, ("dom", "fault")),
            P(("dom", "fault")),
            P("dom"),
            P(None, None, "dom"),
            P(None, "dom"),
            P(None, None, "dom"),
            P(None, None, ("dom", "fault")),
        ),
        out_specs=(P(None, None, ("dom", "fault")), P(None, ("dom", "fault")), P()),
        check_vma=False,
    )
```
